32 devices in a mesh: seq: 8 (over z, x), head: 4 (over y, core).
Axes of the slice: x: 2, y: 2, z: 4, core: 2. Of those that a mesh axis runs over, the one named last changes fastest.
Arguments:
- stream: bfloat16 [4096, 5120], P('seq', 'head'), may hold values from -6 to 6
- gate_input: bfloat16 [4096, 5120], P('seq', 'head'), may hold values from -6 to 6
- in_coeff: bfloat16 [4096, 128], P('seq'), may hold values from -0.5 to 0.5
- out_coeff: bfloat16 [4096, 128], P('seq'), may hold values from -0.5 to 0.5
- step_raw: float32 [80, 4096], P('head', 'seq'), may hold values from -4 to 4
- step_bias: float32 [80], P('head'), may hold values from -1 to 1
- decay_rate: float32 [80], P('head'), may hold values from 0.00024414062 to 0.05
- skip_scale: float32 [80], P('head'), may hold values from 0.5 to 5
- norm_gain: float32 [5120], P('head'), may hold values from 0.1 to 1.9
- out_proj: bfloat16 [5120, 2560], P('head'), may hold values from -0.078125 to 0.078125
- doc_starts: int32 [16], replicated, may hold values from 0 to 4095, as said below
Outputs:
- layer_out: bfloat16 [4096, 2560], P(('seq', 'head'))
The draws below stay inside these ranges and needn't reach their ends.
Inputs may be any that keep to these rules, and one draw needn't show every extreme that they name: `doc_starts`: the first entry is 0, the last is 4095, and the entries strictly increase; entry i is the position where document i begins.
All inputs are finite; a program needn't handle non-finite values.
Results may differ from the reference program's by a relative error of at most 0.01.
Values may be sent and summed in bfloat16 or wider, within the bound.
A program may use at most 128 MiB of HBM per device.

```python
import math
import jax
import jax.numpy as jnp
from jax import lax

D = 2560
HEADS = 80
HEAD_DIM = 64
STATE = 128
DI = 5120
BLOCK = 256
TOKENS = 4096
DOCS = 16
N_HEAD = 4


def draw_decay_rate(key, part):
    pick_key = jax.random.fold_in(key, 101)
    slow_key = jax.random.fold_in(key, 102)
    fast_key = jax.random.fold_in(key, 103)
    slow_share = 0.5
    slow_pick = jax.random.uniform(pick_key, (HEADS,), jnp.float32) < slow_share
    slow_rate = jnp.exp(jax.random.uniform(slow_key, (HEADS,), jnp.float32, 0.0, math.log(2.5))) / TOKENS
    fast_rate = jnp.exp(jax.random.uniform(fast_key, (HEADS,), jnp.float32, math.log(0.01), math.log(0.05)))
    return jnp.where(slow_pick, slow_rate, fast_rate).astype(jnp.float32)


def draw_skip_scale(key, part):
    noise_key = jax.random.fold_in(key, 201)
    ramp_line = 1.0 + 2.0 * jnp.arange(HEADS, dtype=jnp.float32) / max(HEADS - 1, 1)
    noise = jax.random.uniform(noise_key, (HEADS,), jnp.float32, 0.6, 1.4)
    return (ramp_line * noise).astype(jnp.float32)


def draw_doc_starts(key, part):
    quarter_span = TOKENS // 4
    cut_key = jax.random.fold_in(key, 301)
    shuffled = jax.random.permutation(cut_key, quarter_span) + quarter_span
    cuts = jnp.sort(shuffled[:DOCS - 2]).astype(jnp.int32)
    first_one = jnp.zeros((1,), jnp.int32)
    last_one = jnp.full((1,), TOKENS - 1, jnp.int32)
    return jnp.concatenate([first_one, cuts, last_one]).astype(jnp.int32)


def block_scale(key, dims, shards, least, top_value):
    def one(axis_at, blocks):
        heights = jax.random.uniform(jax.random.fold_in(jax.random.fold_in(key, 6), axis_at), (blocks,), jnp.float32, least / len(shards), top_value / len(shards))
        return jnp.repeat(jnp.exp(heights), dims[axis_at] // blocks).reshape((-1,) + (1,) * (len(dims) - axis_at - 1))

    level = one(*shards[0])
    for cut in shards[1:]:
        level = level * one(*cut)
    return level


def gaussian(key, extent, spread, limit, cuts=(), held_as=jnp.bfloat16):
    array = spread * jax.random.normal(key, extent, jnp.float32)
    if cuts:
        array = array * block_scale(key, extent, cuts, -0.22, 0.18)
    return jnp.clip(array, -limit, limit).astype(held_as)


def setup_inputs(seed: int = 0) -> dict:
    key_list = jax.random.split(jax.random.key(seed), 12)
    return {
        "stream": gaussian(key_list[0], (TOKENS, DI), 1.0, 6.0, ((0, 8), (1, 4))),
        "gate_input": gaussian(key_list[1], (TOKENS, DI), 1.0, 6.0, ((0, 8), (1, 4))),
        "in_coeff": gaussian(key_list[2], (TOKENS, STATE), STATE ** -0.5, 0.5, ((0, 8),)),
        "out_coeff": gaussian(key_list[3], (TOKENS, STATE), STATE ** -0.5, 0.5, ((0, 8),)),
        "step_raw": gaussian(key_list[4], (HEADS, TOKENS), 1.0, 4.0, ((0, 4), (1, 8)), jnp.float32),
        "step_bias": jnp.clip(jax.random.uniform(key_list[5], (HEADS,), jnp.float32, -1.0, 1.0) * block_scale(key_list[5], (HEADS,), ((0, 4),), -0.4, 0.0), -1.0, 1.0),
        "decay_rate": draw_decay_rate(jax.random.fold_in(key_list[11], 71), 0),
        "skip_scale": draw_skip_scale(jax.random.fold_in(key_list[11], 71), 0),
        "norm_gain": jnp.clip(1.0 + 0.18 * jax.random.normal(key_list[8], (DI,), jnp.float32), 0.1, 1.9),
        "out_proj": gaussian(key_list[9], (DI, D), DI ** -0.5, 0.078125, ((0, 4),)),
        "doc_starts": draw_doc_starts(jax.random.fold_in(key_list[11], 71), 0),
    }


EPSILON = 1e-05
HIGHEST = lax.Precision.HIGHEST

def block_pass(carry_state, block_piece):
    stream_blk, in_blk, out_blk, step_blk, log_blk, doc_blk, before = block_piece
    head_count = step_blk.shape[0]
    span = step_blk.shape[1]
    head_size = stream_blk.shape[1] // head_count
    index_row = lax.iota(jnp.int32, span)
    upper_ones = (index_row[:, None] <= index_row[None, :]).astype(jnp.float32)
    cumulative = jnp.dot(log_blk, upper_ones, precision=HIGHEST)
    last_cum = cumulative[:, -1]
    same_end = (doc_blk == doc_blk[-1]).astype(jnp.float32)
    end_weight = jnp.exp(jnp.minimum(last_cum[:, None] - cumulative, 0.0)) * step_blk * same_end[None, :]
    scaled_in = (end_weight[:, :, None] * in_blk.astype(jnp.float32)[None, :, :]).astype(jnp.bfloat16)
    values = stream_blk.reshape(span, head_count, head_size)
    fresh_state = jnp.einsum('hsn,shp->hnp', scaled_in.astype(jnp.float32), values.astype(jnp.float32), precision=HIGHEST)
    joined = doc_blk == before
    carry_gate = jnp.where(joined[-1], jnp.exp(last_cum), 0.0)
    new_state = carry_gate[:, None, None] * carry_state + fresh_state
    scores = jnp.dot(out_blk, in_blk.T, preferred_element_type=jnp.float32)
    live_pairs = (doc_blk[:, None] == doc_blk[None, :]) & (index_row[:, None] >= index_row[None, :])
    decay_pairs = jnp.where(live_pairs[None], jnp.exp(jnp.minimum(cumulative[:, :, None] - cumulative[:, None, :], 0.0)), 0.0)
    weights = (scores[None] * decay_pairs * step_blk[:, None, :]).astype(jnp.bfloat16)
    within = jnp.einsum('hts,shp->thp', weights.astype(jnp.float32), values.astype(jnp.float32), precision=HIGHEST)
    carried = jnp.einsum('tn,hnp->thp', out_blk.astype(jnp.float32), carry_state, precision=HIGHEST)
    factor = jnp.where(joined[None, :], jnp.exp(cumulative), 0.0)
    output = within + factor.T[:, :, None] * carried
    return (new_state, output)

def reference(stream, gate_input, in_coeff, out_coeff, step_raw, step_bias, decay_rate, skip_scale, norm_gain, out_proj, doc_starts):
    position = lax.iota(jnp.int32, TOKENS)
    doc_ids = lax.optimization_barrier(jnp.sum((doc_starts[None, :] <= position[:, None]).astype(jnp.int32), axis=1)) - 1
    step_size = jax.nn.softplus(step_raw + step_bias[:, None])
    log_decay = -step_size * decay_rate[:, None]
    block_count = TOKENS // BLOCK
    block_docs = doc_ids.reshape(block_count, BLOCK)
    block_before = jnp.concatenate([jnp.full((1,), -1, jnp.int32), block_docs[:-1, -1]])
    pieces = (stream.reshape(block_count, BLOCK, DI), in_coeff.reshape(block_count, BLOCK, STATE), out_coeff.reshape(block_count, BLOCK, STATE), step_size.reshape(HEADS, block_count, BLOCK).transpose(1, 0, 2), log_decay.reshape(HEADS, block_count, BLOCK).transpose(1, 0, 2), block_docs, block_before)
    zero_state = jnp.zeros((HEADS, STATE, HEAD_DIM), jnp.float32)
    last_state, outputs = lax.scan(block_pass, zero_state, pieces)
    ssm_out = outputs.reshape(TOKENS, HEADS, HEAD_DIM) + skip_scale[None, :, None] * stream.reshape(TOKENS, HEADS, HEAD_DIM).astype(jnp.float32)
    gated = ssm_out.reshape(TOKENS, DI) * jax.nn.silu(gate_input.astype(jnp.float32))
    scale_row = lax.rsqrt(lax.optimization_barrier(jnp.sum(gated * gated, axis=1)) / DI + EPSILON)
    hidden = (gated * scale_row[:, None] * norm_gain[None, :]).astype(jnp.bfloat16)
    group_width = DI // N_HEAD
    summed = jnp.zeros((TOKENS, D), jnp.float32)
    for group_index in range(N_HEAD):
        low = group_index * group_width
        part_sum = jnp.dot(hidden[:, low:low + group_width], out_proj[low:low + group_width, :], preferred_element_type=jnp.float32)
        summed = summed + lax.optimization_barrier(part_sum.astype(jnp.bfloat16)).astype(jnp.float32)
    return summed.astype(jnp.bfloat16)
```

```python
import functools

import jax
import jax.numpy as jnp
from jax import lax
from jax.experimental import pallas as pl
from jax.experimental.pallas import tpu as pltpu
from jax.sharding import PartitionSpec as P

EPSILON = 1e-05
F32 = jnp.float32
BF16 = jnp.bfloat16
MESH = pl.DeviceIdType.MESH
LAG = 2
SPLIT = 2
FAR_LAG = 2


def dot(a, b, ca, cb):
    return lax.dot_general(a, b, (((ca,), (cb,)), ((), ())), preferred_element_type=F32)


def split(value, parts):
    pieces = []
    for _ in range(parts):
        piece = value.astype(BF16).astype(F32)
        pieces.append(piece)
        value = value - piece
    return jnp.concatenate(pieces, axis=0).astype(BF16)


def to_column(row):
    n = row.shape[1]
    eye = lax.broadcasted_iota(jnp.int32, (n, n), 0) == lax.broadcasted_iota(jnp.int32, (n, n), 1)
    return jnp.sum(jnp.where(eye, row, 0.0), axis=1, keepdims=True)


def kernel(
    n_seq,
    n_head,
    heads,
    chunks,
    pieces,
    starts_hbm,
    step_hbm,
    bias_hbm,
    rate_hbm,
    skip_hbm,
    gain_hbm,
    in_hbm,
    out_hbm,
    stream_hbm,
    gate_hbm,
    proj_hbm,
    result_ref,
    starts_ref,
    step_ref,
    bias_ref,
    rate_ref,
    skip_ref,
    gain_ref,
    in_ref,
    out_ref,
    stream,
    gate,
    proj,
    pad,
    expand,
    factor_in,
    factor_out,
    pairs,
    carry_in,
    source,
    summary,
    link_own,
    link_prev,
    before_gate,
    base,
    slope,
    square,
    hidden,
    chain_out,
    chain_in,
    cross_in,
    square_out,
    square_in,
    held,
    near_out,
    near_in,
    far_out,
    far_in,
    small_sem,
    load_sem,
    link_sem,
    chain_sem,
    cross_sem,
    square_sem,
    near_sem,
    far_sem,
):
    rows, channels = stream.shape
    state = in_ref.shape[1]
    width = channels // chunks
    head_size = channels // heads
    padded = pad.shape[0]
    sub = width // SPLIT
    half = rows // 2
    share = rows // n_head
    piece = proj.shape[1] // pieces

    s = lax.axis_index("seq")
    g = lax.axis_index("head")
    parity = s % 2
    pair = s // 2
    last_pair = n_seq // 2 - 1
    core = g % 2
    side = g // 2
    near = side * 2 + (1 - core)
    far = (1 - side) * 2 + core
    cross = s + 1 - 2 * parity
    peers = (near, far, (1 - side) * 2 + (1 - core))

    loads = [
        pltpu.make_async_copy(src, dst, load_sem.at[i])
        for i, (src, dst) in enumerate(((stream_hbm, stream), (gate_hbm, gate), (proj_hbm, proj)))
    ]
    smalls = [
        pltpu.make_async_copy(src, dst, small_sem.at[i])
        for i, (src, dst) in enumerate(
            (
                (step_hbm, step_ref),
                (bias_hbm, bias_ref),
                (rate_hbm, rate_ref),
                (starts_hbm, starts_ref),
                (in_hbm, in_ref),
                (skip_hbm, skip_ref),
                (gain_hbm, gain_ref),
                (out_hbm, out_ref),
            )
        )
    ]
    for small in smalls[:3]:
        small.start()
    loads[0].start()
    for small in smalls[3:]:
        small.start()

    barrier = pltpu.get_barrier_semaphore()
    greeted = [(s >= 2, s - 2), (s >= 1, s - 1), (s + 1 < n_seq, s + 1), (s + 2 < n_seq, s + 2)]
    for there, other in greeted:

        @pl.when(there)
        def _(other=other):
            pl.semaphore_signal(barrier, inc=1, device_id=(other, g), device_id_type=MESH)

    for peer in peers:
        pl.semaphore_signal(barrier, inc=1, device_id=(s, peer), device_id_type=MESH)
    greetings = len(peers) + sum(there.astype(jnp.int32) for there, _ in greeted)

    def send(src, dst, sems, seq, head):
        return pltpu.make_async_remote_copy(
            src_ref=src,
            dst_ref=dst,
            send_sem=sems.at[0],
            recv_sem=sems.at[1],
            device_id=(seq, head),
            device_id_type=MESH,
        )

    link_copy = send(link_own, link_prev, link_sem, (s + 1) % n_seq, g)

    def chain_copy(k):
        return send(
            chain_out.at[k], chain_in.at[k], chain_sem.at[k], (s + 2) % n_seq, g
        )

    def cross_copy(k, even):
        source_ref = chain_out if even else chain_in
        return send(source_ref.at[k], cross_in.at[k], cross_sem.at[k], cross, g)

    pad[...] = jnp.zeros_like(pad)
    for small in smalls:
        small.wait()
    raw = step_ref[...] + to_column(bias_ref[...])
    pad[pl.ds(0, heads), :] = jnp.maximum(raw, 0.0) + jnp.log(1.0 + jnp.exp(-jnp.abs(raw)))
    step_size = pad[...]
    head_row = lax.broadcasted_iota(jnp.int32, (padded, channels), 0) * head_size
    lane = lax.broadcasted_iota(jnp.int32, (padded, channels), 1)
    spread = jnp.where((lane >= head_row) & (lane < head_row + head_size), 1.0, 0.0)
    expand[...] = jnp.concatenate([spread, spread], axis=0).astype(BF16)
    rate = to_column(rate_ref[...])
    if padded > heads:
        rate = jnp.concatenate([rate, jnp.zeros((padded - heads, 1), F32)], axis=0)
    log_decay = -step_size * rate
    first = lax.broadcasted_iota(jnp.int32, (rows, rows), 0)
    second = lax.broadcasted_iota(jnp.int32, (rows, rows), 1)
    upper = jnp.where(first <= second, 1.0, 0.0).astype(BF16)
    sums = dot(split(log_decay, 3), upper, 1, 0)
    cumulative = sums[:padded] + sums[padded : 2 * padded] + sums[2 * padded :]
    middle = cumulative[:, half - 1 : half]
    last = cumulative[:, rows - 1 : rows]
    factor_in[...] = split(jnp.exp(middle - cumulative) * step_size, 2)

    starts = starts_ref[...].astype(F32).reshape(1, -1)
    offset = s * rows
    place = (offset + lax.broadcasted_iota(jnp.int32, (rows, 1), 0)).astype(F32)
    place_lane = (offset + lax.broadcasted_iota(jnp.int32, (1, rows), 1)).astype(F32)
    doc = jnp.sum(jnp.where(starts <= place, 1.0, 0.0), axis=1, keepdims=True)
    before = jnp.sum(jnp.where(starts <= (offset - 1).astype(F32), 1.0, 0.0), axis=1, keepdims=True)
    doc_end = doc[rows - 1 : rows, :]
    joined_end = jnp.where(doc_end == before, 1.0, 0.0)

    def per_channel(column):
        return jnp.sum(spread * column, axis=0, keepdims=True)

    link_own[...] = per_channel(jnp.exp(last)) * joined_end
    end_gate = per_channel(jnp.exp(last - middle))
    before_gate[1:2, :] = end_gate
    in_end = jnp.where(doc == doc_end, in_ref[...].astype(F32), 0.0).astype(BF16)

    pl.semaphore_wait(barrier, greetings)

    @pl.when(s < n_seq - 1)
    def _():
        link_copy.start()

    loads[0].wait()
    loads[1].start()
    loads[2].start()

    def columns(k):
        return pl.ds(pl.multiple_of(k * width, width), width)

    def make_summary(k, _):
        cols = columns(k)
        scale = dot(factor_in[...], expand[:, cols], 0, 0)
        scaled = (stream[:, cols].astype(F32) * scale).astype(BF16)
        source[:, cols] = scaled
        fresh = dot(in_end, scaled, 0, 0) * before_gate[1:2, cols]

        @pl.when(pair == 0)
        def _():
            for i in range(SPLIT):
                at = k * SPLIT + i
                chain_out[at] = fresh[:, i * sub : (i + 1) * sub].astype(BF16)
                chain_in[at] = jnp.zeros((state, sub), BF16)
                if last_pair > 0:
                    chain_copy(at).start()

                @pl.when(parity == 0)
                def _():
                    cross_in[at] = jnp.zeros((state, sub), BF16)
                    cross_copy(at, True).start()

        @pl.when(pair > 0)
        def _():
            for i in range(SPLIT):
                summary[k * SPLIT + i] = fresh[:, i * sub : (i + 1) * sub]

        return 0

    lax.fori_loop(0, chunks, make_summary, 0)

    factor_out[...] = split(jnp.exp(cumulative - middle), 2)
    before_gate[3:4, :] = gain_ref[...].reshape(1, -1)
    doc_lane = jnp.sum(jnp.where(to_column(starts) <= place_lane, 1.0, 0.0), axis=0, keepdims=True)
    before_gate[0:1, :] = per_channel(jnp.exp(middle))
    skip = to_column(skip_ref[...])
    if padded > heads:
        skip = jnp.concatenate([skip, jnp.zeros((padded - heads, 1), F32)], axis=0)
    before_gate[2:3, :] = per_channel(skip)
    carry_in[...] = jnp.where(doc == before, out_ref[...].astype(F32), 0.0).astype(BF16)
    scores = dot(out_ref[...], in_ref[...], 1, 1)
    live = (first >= second) & (doc == doc_lane)
    pairs[...] = jnp.where(live, scores, 0.0).astype(BF16)
    square[...] = jnp.zeros_like(square)
    loads[1].wait()

    @pl.when(s > 0)
    def _():
        link_copy.wait_recv()

    @pl.when(s == 0)
    def _():
        link_prev[...] = jnp.zeros_like(link_prev)

    def local_part(k):
        cols = columns(k)
        gate_value = gate[:, cols].astype(F32)
        silu = gate_value * (0.5 * jnp.tanh(0.5 * gate_value) + 0.5)
        within = jnp.concatenate(
            [
                dot(pairs[:half, :half], source[:half, cols], 1, 0),
                dot(pairs[half:, :], source[:, cols], 1, 0),
            ],
            axis=0,
        )
        factor = dot(factor_out[...], expand[:, cols], 0, 0) * silu
        slope[:, cols] = factor
        base[:, cols] = within * factor + stream[:, cols].astype(F32) * before_gate[2:3, cols] * silu

    def forward(k):
        @pl.when(pair > 0)
        def _():
            chain_copy(k).wait_recv()

            @pl.when(parity == 1)
            def _():
                cross_copy(k, False).start()

            cols = pl.ds(pl.multiple_of(k * sub, sub), sub)
            longer = link_own[:, cols] * link_prev[:, cols] * chain_in[k].astype(F32)
            chain_out[k] = (longer + summary[k]).astype(BF16)

            @pl.when(pair < last_pair)
            def _():
                chain_copy(k).start()

            @pl.when(parity == 0)
            def _():
                cross_copy(k, True).start()

    def finish(k):
        @pl.when(s > 0)
        def _():
            for i in range(SPLIT):
                cross_copy(k * SPLIT + i, True).wait_recv()

        cols = columns(k)
        own = jnp.concatenate([chain_in[k * SPLIT + i].astype(F32) for i in range(SPLIT)], axis=1)
        other = jnp.concatenate([cross_in[k * SPLIT + i].astype(F32) for i in range(SPLIT)], axis=1)
        incoming = link_prev[:, cols] * own + other
        incoming = (incoming * before_gate[0:1, cols]).astype(BF16)
        carried = dot(carry_in[...], incoming, 1, 0)
        gated = base[:, cols] + slope[:, cols] * carried
        hidden[:, cols] = (gated * before_gate[3:4, cols]).astype(BF16)
        squares = gated * gated
        total = square[...]
        for i in range(width // 128):
            total = total + squares[:, i * 128 : (i + 1) * 128]
        square[...] = total

    def main_step(k, _):
        @pl.when(k < chunks)
        def _():
            local_part(k)
            for i in range(SPLIT):
                forward(k * SPLIT + i)

        @pl.when(k >= LAG)
        def _():
            finish(k - LAG)

        return 0

    lax.fori_loop(0, chunks + LAG, main_step, 0)

    loads[2].wait()

    def piece_columns(j):
        return pl.ds(pl.multiple_of(j * piece, piece), piece)

    def near_copy(stage, j):
        at = stage * pieces + j
        return send(near_out.at[at], near_in.at[at], near_sem.at[at], s, near)

    def far_copy(j):
        return send(far_out.at[j], far_in.at[j], far_sem.at[j], s, far)

    def half_rows(which):
        return pl.ds(pl.multiple_of(which * 2 * share, 2 * share), 2 * share)

    def core_rows(which):
        return pl.ds(pl.multiple_of(which * share, share), share)

    def project(stage, which, j):
        held[stage * pieces + j] = dot(hidden[half_rows(which), :], proj[:, piece_columns(j)], 1, 0)
        near_out[stage * pieces + j] = held[stage * pieces + j, core_rows(1 - core), :].astype(BF16)
        near_copy(stage, j).start()

    def pass_on(j):
        near_copy(0, j).wait_recv()
        both = held[j, core_rows(core), :] + near_in[j].astype(F32)
        far_out[j] = both.astype(BF16)
        far_copy(j).start()

    def square_copy(i):
        return send(square_out.at[peers[i]], square_in.at[i], square_sem.at[i], s, peers[i])

    def send_squares():
        for owner in range(n_head):
            block = square[owner * share : (owner + 1) * share, :]
            sums_lane = jnp.sum(block.T, axis=0, keepdims=True)
            square_out[owner] = jnp.broadcast_to(sums_lane, (8, share))
        for i in range(len(peers)):
            square_copy(i).start()

    def far_step(j, _):
        @pl.when(j < pieces)
        def _():
            project(0, 1 - side, j)

        @pl.when(j >= FAR_LAG)
        def _():
            pass_on(j - FAR_LAG)

        @pl.when(j == FAR_LAG)
        def _():
            send_squares()

        return 0

    lax.fori_loop(0, pieces + FAR_LAG, far_step, 0)

    def near_step(j, _):
        project(1, side, j)
        return 0

    lax.fori_loop(0, pieces, near_step, 0)

    total = square_out[g]
    for i in range(len(peers)):
        square_copy(i).wait()
        total = total + square_in[i]
    mean = jnp.broadcast_to(total[0:1, :], (128, share)).T / (channels * n_head)
    scale_row = lax.rsqrt(mean + EPSILON)[:, 0:1]

    def collect(j, _):
        near_copy(1, j).wait_recv()
        far_copy(j).wait_recv()
        at = pieces + j
        whole = held[at, core_rows(core), :] + near_in[at].astype(F32) + far_in[j].astype(F32)
        result_ref[:, piece_columns(j)] = (whole * scale_row).astype(BF16)
        return 0

    lax.fori_loop(0, pieces, collect, 0)

    @pl.when(s < n_seq - 1)
    def _():
        link_copy.wait_send()

    def drain(k, _):
        @pl.when(pair < last_pair)
        def _():
            chain_copy(k).wait_send()

        @pl.when(parity == 0)
        def _():
            cross_copy(k, True).wait_send()

        @pl.when((parity == 1) & (pair > 0))
        def _():
            cross_copy(k, False).wait_send()

        return 0

    lax.fori_loop(0, chunks * SPLIT, drain, 0)

    def drain_pieces(j, _):
        near_copy(0, j).wait_send()
        near_copy(1, j).wait_send()
        far_copy(j).wait_send()
        return 0

    lax.fori_loop(0, pieces, drain_pieces, 0)


def local(
    n_seq,
    n_head,
    stream,
    gate_input,
    in_coeff,
    out_coeff,
    step_raw,
    step_bias,
    decay_rate,
    skip_scale,
    norm_gain,
    out_proj,
    doc_starts,
):
    rows, channels = stream.shape
    heads = step_raw.shape[0]
    state = in_coeff.shape[1]
    model = out_proj.shape[1]
    chunks, pieces = channels // 256, model // 256
    width, piece = channels // chunks, model // pieces
    parts, sub = chunks * SPLIT, width // SPLIT
    padded = -(-heads // 8) * 8
    share = rows // n_head
    assert n_head == 4 and n_seq % 2 == 0 and rows <= 512
    vmem = pl.BlockSpec(memory_space=pltpu.VMEM)
    anywhere = pl.BlockSpec(memory_space=pl.ANY)
    dma = pltpu.SemaphoreType.DMA
    return pl.pallas_call(
        functools.partial(kernel, n_seq, n_head, heads, chunks, pieces),
        out_shape=pltpu.VMEM((share, model), BF16),
        in_specs=[anywhere] * 11,
        out_specs=vmem,
        scratch_shapes=[
            pltpu.VMEM(doc_starts.shape, doc_starts.dtype),
            pltpu.VMEM(step_raw.shape, F32),
            pltpu.VMEM((1, heads), F32),
            pltpu.VMEM((1, heads), F32),
            pltpu.VMEM((1, heads), F32),
            pltpu.VMEM(norm_gain.shape, F32),
            pltpu.VMEM(in_coeff.shape, BF16),
            pltpu.VMEM(out_coeff.shape, BF16),
            pltpu.VMEM((rows, channels), BF16),
            pltpu.VMEM((rows, channels), BF16),
            pltpu.VMEM((channels, model), BF16),
            pltpu.VMEM((padded, rows), F32),
            pltpu.VMEM((2 * padded, channels), BF16),
            pltpu.VMEM((2 * padded, rows), BF16),
            pltpu.VMEM((2 * padded, rows), BF16),
            pltpu.VMEM((rows, rows), BF16),
            pltpu.VMEM((rows, state), BF16),
            pltpu.VMEM((rows, channels), BF16),
            pltpu.VMEM((parts, state, sub), F32),
            pltpu.VMEM((1, channels), F32),
            pltpu.VMEM((1, channels), F32),
            pltpu.VMEM((8, channels), F32),
            pltpu.VMEM((rows, channels), F32),
            pltpu.VMEM((rows, channels), F32),
            pltpu.VMEM((rows, 128), F32),
            pltpu.VMEM((rows, channels), BF16),
            pltpu.VMEM((parts, state, sub), BF16),
            pltpu.VMEM((parts, state, sub), BF16),
            pltpu.VMEM((parts, state, sub), BF16),
            pltpu.VMEM((n_head, 8, share), F32),
            pltpu.VMEM((n_head - 1, 8, share), F32),
            pltpu.VMEM((2 * pieces, 2 * share, piece), F32),
            pltpu.VMEM((2 * pieces, share, piece), BF16),
            pltpu.VMEM((2 * pieces, share, piece), BF16),
            pltpu.VMEM((pieces, share, piece), BF16),
            pltpu.VMEM((pieces, share, piece), BF16),
            dma((8,)),
            dma((3,)),
            dma((2,)),
            dma((parts, 2)),
            dma((parts, 2)),
            dma((n_head - 1, 2)),
            dma((2 * pieces, 2)),
            dma((pieces, 2)),
        ],
        compiler_params=pltpu.CompilerParams(
            collective_id=0, has_side_effects=True, vmem_limit_bytes=56 * 1024 * 1024
        ),
    )(
        doc_starts,
        step_raw,
        step_bias.reshape(1, -1),
        decay_rate.reshape(1, -1),
        skip_scale.reshape(1, -1),
        norm_gain,
        in_coeff,
        out_coeff,
        stream,
        gate_input,
        out_proj,
    )


def solution(mesh):
    in_specs = (
        P("seq", "head"),
        P("seq", "head"),
        P("seq", None),
        P("seq", None),
        P("head", "seq"),
        P("head"),
        P("head"),
        P("head"),
        P("head"),
        P("head", None),
        P(),
    )
    out_specs = P(("seq", "head"), None)
    body = functools.partial(local, mesh.shape["seq"], mesh.shape["head"])
    return jax.shard_map(body, mesh=mesh, in_specs=in_specs, out_specs=out_specs, check_vma=False)
```

```python
import functools

import jax
import jax.numpy as jnp
from jax import lax
from jax.experimental import pallas as pl
from jax.experimental.pallas import tpu as pltpu
from jax.sharding import PartitionSpec as P

EPSILON = 1e-05
F32 = jnp.float32
BF16 = jnp.bfloat16
MESH = pl.DeviceIdType.MESH
EARLY = 1
FAR_LAG = 2


def dot(a, b, ca, cb):
    return lax.dot_general(a, b, (((ca,), (cb,)), ((), ())), preferred_element_type=F32)


def split(value, parts):
    pieces = []
    for _ in range(parts):
        piece = value.astype(BF16).astype(F32)
        pieces.append(piece)
        value = value - piece
    return jnp.concatenate(pieces, axis=0).astype(BF16)


def to_column(row):
    n = row.shape[1]
    eye = lax.broadcasted_iota(jnp.int32, (n, n), 0) == lax.broadcasted_iota(jnp.int32, (n, n), 1)
    return jnp.sum(jnp.where(eye, row, 0.0), axis=1, keepdims=True)


def kernel(
    n_seq,
    n_head,
    heads,
    chunks,
    pieces,
    starts_hbm,
    step_hbm,
    bias_hbm,
    rate_hbm,
    skip_hbm,
    gain_hbm,
    in_hbm,
    out_hbm,
    stream_hbm,
    gate_hbm,
    proj_hbm,
    result_ref,
    starts_ref,
    step_ref,
    bias_ref,
    rate_ref,
    skip_ref,
    gain_ref,
    in_ref,
    out_ref,
    stream,
    gate,
    proj,
    pad,
    expand,
    factor_in,
    factor_out,
    pairs,
    carry_in,
    source,
    link_own,
    link_all,
    before_gate,
    base,
    slope,
    square,
    hidden,
    fresh_own,
    fresh_all,
    chain_out,
    states,
    incoming_all,
    square_out,
    square_in,
    held,
    near_out,
    near_in,
    far_out,
    far_in,
    small_sem,
    load_sem,
    ready_sem,
    link_send,
    link_recv,
    fresh_send,
    fresh_recv,
    chain_sem,
    return_send,
    return_recv,
    square_sem,
    near_sem,
    far_sem,
):
    rows, channels = stream.shape
    state = in_ref.shape[1]
    width = channels // chunks
    head_size = channels // heads
    padded = pad.shape[0]
    sub = width // 2
    half = rows // 2
    share = rows // n_head
    piece = proj.shape[1] // pieces

    s = lax.axis_index("seq")
    g = lax.axis_index("head")
    parity = s % 2
    pair = s // 2
    last_pair = n_seq // 2 - 1
    core = g % 2
    side = g // 2
    near = side * 2 + (1 - core)
    far = (1 - side) * 2 + core
    cross = s + 1 - 2 * parity
    carrier = 2 * side + 1
    carries = core == 1
    peers = (near, far, (1 - side) * 2 + (1 - core))

    loads = [
        pltpu.make_async_copy(src, dst, load_sem.at[i])
        for i, (src, dst) in enumerate(((stream_hbm, stream), (gate_hbm, gate), (proj_hbm, proj)))
    ]
    smalls = [
        pltpu.make_async_copy(src, dst, small_sem.at[i])
        for i, (src, dst) in enumerate(
            (
                (step_hbm, step_ref),
                (bias_hbm, bias_ref),
                (rate_hbm, rate_ref),
                (starts_hbm, starts_ref),
                (in_hbm, in_ref),
                (skip_hbm, skip_ref),
                (gain_hbm, gain_ref),
                (out_hbm, out_ref),
            )
        )
    ]
    for small in smalls[:3]:
        small.start()
    loads[0].start()
    for small in smalls[3:]:
        small.start()

    barrier = pltpu.get_barrier_semaphore()
    for peer in peers:
        pl.semaphore_signal(barrier, inc=1, device_id=(s, peer), device_id_type=MESH)
    for peer in (g, near):
        pl.semaphore_signal(barrier, inc=1, device_id=(cross, peer), device_id_type=MESH)

    @pl.when(pair < last_pair)
    def _():
        pl.semaphore_signal(barrier, inc=1, device_id=(s + 2, g), device_id_type=MESH)

    def remote(src, dst, send_sem, recv_sem, seq, head):
        return pltpu.make_async_remote_copy(
            src_ref=src,
            dst_ref=dst,
            send_sem=send_sem,
            recv_sem=recv_sem,
            device_id=(seq, head),
            device_id_type=MESH,
        )

    def send(src, dst, sems, seq, head):
        return remote(src, dst, sems.at[0], sems.at[1], seq, head)

    def link_copy(away, shard, part):
        return remote(
            link_own,
            link_all.at[shard, part],
            link_send.at[away],
            link_recv.at[shard, part],
            cross if away else s,
            carrier,
        )

    def fresh_copy(k, away, shard, part):
        return remote(
            fresh_own.at[k, 1 - parity if away else parity],
            fresh_all.at[shard, part, k],
            fresh_send.at[away, k],
            fresh_recv.at[shard, part, k],
            cross if away else s,
            carrier,
        )

    def chain_copy(k, part):
        return send(
            chain_out.at[k, part], states.at[0, k, part], chain_sem.at[k, part], (s + 2) % n_seq, g
        )

    def return_copy(k, away, part, owner):
        return remote(
            states.at[1 - parity if away else parity, k, part],
            incoming_all.at[k, owner],
            return_send.at[k, away, part],
            return_recv.at[k, owner],
            cross if away else s,
            2 * side + part,
        )

    pad[...] = jnp.zeros_like(pad)
    for small in smalls:
        small.wait()
    pl.semaphore_wait(barrier, len(peers) + 2 + (pair > 0).astype(jnp.int32))

    @pl.when(carries & (pair > 0))
    def _():
        pl.semaphore_signal(ready_sem, inc=1, device_id=(s - 2, g), device_id_type=MESH)

    raw = step_ref[...] + to_column(bias_ref[...])
    pad[pl.ds(0, heads), :] = jnp.maximum(raw, 0.0) + jnp.log(1.0 + jnp.exp(-jnp.abs(raw)))
    step_size = pad[...]
    head_row = lax.broadcasted_iota(jnp.int32, (padded, channels), 0) * head_size
    lane = lax.broadcasted_iota(jnp.int32, (padded, channels), 1)
    spread = jnp.where((lane >= head_row) & (lane < head_row + head_size), 1.0, 0.0)
    expand[...] = jnp.concatenate([spread, spread], axis=0).astype(BF16)
    rate = to_column(rate_ref[...])
    if padded > heads:
        rate = jnp.concatenate([rate, jnp.zeros((padded - heads, 1), F32)], axis=0)
    log_decay = -step_size * rate
    first = lax.broadcasted_iota(jnp.int32, (rows, rows), 0)
    second = lax.broadcasted_iota(jnp.int32, (rows, rows), 1)
    upper = jnp.where(first <= second, 1.0, 0.0).astype(BF16)
    sums = dot(split(log_decay, 3), upper, 1, 0)
    cumulative = sums[:padded] + sums[padded : 2 * padded] + sums[2 * padded :]
    middle = cumulative[:, half - 1 : half]
    last = cumulative[:, rows - 1 : rows]
    factor_in[...] = split(jnp.exp(middle - cumulative) * step_size, 2)

    starts = starts_ref[...].astype(F32).reshape(1, -1)
    offset = s * rows
    place = (offset + lax.broadcasted_iota(jnp.int32, (rows, 1), 0)).astype(F32)
    place_lane = (offset + lax.broadcasted_iota(jnp.int32, (1, rows), 1)).astype(F32)
    doc = jnp.sum(jnp.where(starts <= place, 1.0, 0.0), axis=1, keepdims=True)
    before = jnp.sum(jnp.where(starts <= (offset - 1).astype(F32), 1.0, 0.0), axis=1, keepdims=True)
    doc_end = doc[rows - 1 : rows, :]
    joined_end = jnp.where(doc_end == before, 1.0, 0.0)

    def per_channel(column):
        return jnp.sum(spread * column, axis=0, keepdims=True)

    link_own[...] = per_channel(jnp.exp(last)) * joined_end
    end_gate = per_channel(jnp.exp(last - middle))
    before_gate[1:2, :] = end_gate
    in_end = jnp.where(doc == doc_end, in_ref[...].astype(F32), 0.0).astype(BF16)

    link_copy(1, parity, core).start()

    @pl.when(core == 0)
    def _():
        link_copy(0, parity, core).start()

    @pl.when(carries)
    def _():
        link_all[parity, 1] = link_own[...]

    loads[0].wait()
    loads[1].start()
    loads[2].start()

    def columns(k):
        return pl.ds(pl.multiple_of(k * width, width), width)

    def make_summary(k, _):
        cols = columns(k)
        scale = dot(factor_in[...], expand[:, cols], 0, 0)
        scaled = (stream[:, cols].astype(F32) * scale).astype(BF16)
        source[:, cols] = scaled
        fresh = dot(in_end, scaled, 0, 0) * before_gate[1:2, cols]

        for i in range(2):
            fresh_own[k, i] = fresh[:, i * sub : (i + 1) * sub].astype(BF16)
        fresh_copy(k, 1, parity, core).start()

        @pl.when(core == 0)
        def _():
            fresh_copy(k, 0, parity, core).start()

        @pl.when(carries)
        def _():
            fresh_all[parity, 1, k] = fresh_own[k, parity]

        return 0

    lax.fori_loop(0, chunks, make_summary, 0)

    factor_out[...] = split(jnp.exp(cumulative - middle), 2)
    before_gate[3:4, :] = gain_ref[...].reshape(1, -1)
    doc_lane = jnp.sum(jnp.where(to_column(starts) <= place_lane, 1.0, 0.0), axis=0, keepdims=True)
    before_gate[0:1, :] = per_channel(jnp.exp(middle))
    skip = to_column(skip_ref[...])
    if padded > heads:
        skip = jnp.concatenate([skip, jnp.zeros((padded - heads, 1), F32)], axis=0)
    before_gate[2:3, :] = per_channel(skip)
    carry_in[...] = jnp.where(doc == before, out_ref[...].astype(F32), 0.0).astype(BF16)
    scores = dot(out_ref[...], in_ref[...], 1, 1)
    live = (first >= second) & (doc == doc_lane)
    pairs[...] = jnp.where(live, scores, 0.0).astype(BF16)
    square[...] = jnp.zeros_like(square)
    loads[1].wait()

    @pl.when(s == 0)
    def _():
        incoming_all[...] = jnp.zeros_like(incoming_all)

    @pl.when(carries)
    def _():
        link_copy(0, parity, 0).wait_recv()
        link_copy(1, 1 - parity, 0).wait_recv()
        link_copy(1, 1 - parity, 1).wait_recv()

    def local_part(k):
        cols = columns(k)
        gate_value = gate[:, cols].astype(F32)
        silu = gate_value * (0.5 * jnp.tanh(0.5 * gate_value) + 0.5)
        within = jnp.concatenate(
            [
                dot(pairs[:half, :half], source[:half, cols], 1, 0),
                dot(pairs[half:, :], source[:, cols], 1, 0),
            ],
            axis=0,
        )
        factor = dot(factor_out[...], expand[:, cols], 0, 0) * silu
        slope[:, cols] = factor
        base[:, cols] = within * factor + stream[:, cols].astype(F32) * before_gate[2:3, cols] * silu

    def chain_step(k):
        cols = pl.ds(pl.multiple_of(k * width + parity * sub, sub), sub)
        fresh_copy(k, 0, parity, 0).wait_recv()
        fresh_copy(k, 1, 1 - parity, 0).wait_recv()
        fresh_copy(k, 1, 1 - parity, 1).wait_recv()

        for part in range(2):
            keep_even, keep_odd = link_all[0, part, :, cols], link_all[1, part, :, cols]
            fresh_even = fresh_all[0, part, k].astype(F32)
            fresh_odd = fresh_all[1, part, k].astype(F32)

            @pl.when(pair > 0)
            def _():
                chain_copy(k, part).wait_recv()
                between = keep_even * states[0, k, part].astype(F32) + fresh_even
                states[1, k, part] = between.astype(BF16)
                chain_out[k, part] = (keep_odd * between + fresh_odd).astype(BF16)

            @pl.when(pair == 0)
            def _():
                states[1, k, part] = fresh_all[0, part, k]
                chain_out[k, part] = (keep_odd * fresh_even + fresh_odd).astype(BF16)

            @pl.when(pair < last_pair)
            def _():
                chain_copy(k, part).start()

            @pl.when(cross > 0)
            def _():
                return_copy(k, 1, part, parity).start()

            @pl.when(s > 0)
            def _():
                if part == 0:
                    return_copy(k, 0, part, parity).start()
                else:
                    incoming_all[k, parity] = states[parity, k, part]

    def finish(k):
        @pl.when(s > 0)
        def _():
            return_copy(k, 1, core, 1 - parity).wait_recv()

            @pl.when(core == 0)
            def _():
                return_copy(k, 0, core, parity).wait_recv()

        cols = columns(k)
        incoming = jnp.concatenate([incoming_all[k, i].astype(F32) for i in range(2)], axis=1)
        incoming = (incoming * before_gate[0:1, cols]).astype(BF16)
        carried = dot(carry_in[...], incoming, 1, 0)
        gated = base[:, cols] + slope[:, cols] * carried
        hidden[:, cols] = (gated * before_gate[3:4, cols]).astype(BF16)
        squares = gated * gated
        total = square[...]
        for i in range(width // 128):
            total = total + squares[:, i * 128 : (i + 1) * 128]
        square[...] = total

    lead = jnp.where(carries & (pair < EARLY), 0, chunks)

    def main_step(step, _):
        @pl.when(carries & (step >= lead) & (step < lead + chunks))
        def _():
            chain_step(step - lead)

        @pl.when(step < chunks)
        def _():
            local_part(step)

        return 0

    @pl.when(carries & (pair < last_pair))
    def _():
        pl.semaphore_wait(ready_sem, 1)

    lax.fori_loop(0, chunks + jnp.where(carries, lead, 0), main_step, 0)

    def finish_step(k, _):
        finish(k)
        return 0

    lax.fori_loop(0, chunks, finish_step, 0)

    loads[2].wait()

    def piece_columns(j):
        return pl.ds(pl.multiple_of(j * piece, piece), piece)

    def near_copy(stage, j):
        at = stage * pieces + j
        return send(near_out.at[at], near_in.at[at], near_sem.at[at], s, near)

    def far_copy(j):
        return send(far_out.at[j], far_in.at[j], far_sem.at[j], s, far)

    def half_rows(which):
        return pl.ds(pl.multiple_of(which * 2 * share, 2 * share), 2 * share)

    def core_rows(which):
        return pl.ds(pl.multiple_of(which * share, share), share)

    def project(stage, which, j):
        held[stage * pieces + j] = dot(hidden[half_rows(which), :], proj[:, piece_columns(j)], 1, 0)
        near_out[stage * pieces + j] = held[stage * pieces + j, core_rows(1 - core), :].astype(BF16)
        near_copy(stage, j).start()

    def pass_on(j):
        near_copy(0, j).wait_recv()
        both = held[j, core_rows(core), :] + near_in[j].astype(F32)
        far_out[j] = both.astype(BF16)
        far_copy(j).start()

    def square_copy(i):
        return send(square_out.at[peers[i]], square_in.at[i], square_sem.at[i], s, peers[i])

    def send_squares():
        for owner in range(n_head):
            block = square[owner * share : (owner + 1) * share, :]
            sums_lane = jnp.sum(block.T, axis=0, keepdims=True)
            square_out[owner] = jnp.broadcast_to(sums_lane, (8, share))
        for i in range(len(peers)):
            square_copy(i).start()

    def far_step(j, _):
        @pl.when(j < pieces)
        def _():
            project(0, 1 - side, j)

        @pl.when(j >= FAR_LAG)
        def _():
            pass_on(j - FAR_LAG)

        @pl.when(j == FAR_LAG)
        def _():
            send_squares()

        return 0

    lax.fori_loop(0, pieces + FAR_LAG, far_step, 0)

    def near_step(j, _):
        project(1, side, j)
        return 0

    lax.fori_loop(0, pieces, near_step, 0)

    total = square_out[g]
    for i in range(len(peers)):
        square_copy(i).wait()
        total = total + square_in[i]
    mean = jnp.broadcast_to(total[0:1, :], (128, share)).T / (channels * n_head)
    scale_row = lax.rsqrt(mean + EPSILON)[:, 0:1]

    def collect(j, _):
        near_copy(1, j).wait_recv()
        far_copy(j).wait_recv()
        at = pieces + j
        whole = held[at, core_rows(core), :] + near_in[at].astype(F32) + far_in[j].astype(F32)
        result_ref[:, piece_columns(j)] = (whole * scale_row).astype(BF16)
        return 0

    lax.fori_loop(0, pieces, collect, 0)

    link_copy(1, parity, core).wait_send()

    @pl.when(core == 0)
    def _():
        link_copy(0, parity, core).wait_send()

    def drain(k, _):
        fresh_copy(k, 1, parity, core).wait_send()

        @pl.when(core == 0)
        def _():
            fresh_copy(k, 0, parity, core).wait_send()

        @pl.when(carries)
        def _():
            for part in range(2):

                @pl.when(pair < last_pair)
                def _():
                    chain_copy(k, part).wait_send()

                @pl.when(cross > 0)
                def _():
                    return_copy(k, 1, part, parity).wait_send()

            @pl.when(s > 0)
            def _():
                return_copy(k, 0, 0, parity).wait_send()

        return 0

    lax.fori_loop(0, chunks, drain, 0)

    def drain_pieces(j, _):
        near_copy(0, j).wait_send()
        near_copy(1, j).wait_send()
        far_copy(j).wait_send()
        return 0

    lax.fori_loop(0, pieces, drain_pieces, 0)


def local(
    n_seq,
    n_head,
    stream,
    gate_input,
    in_coeff,
    out_coeff,
    step_raw,
    step_bias,
    decay_rate,
    skip_scale,
    norm_gain,
    out_proj,
    doc_starts,
):
    rows, channels = stream.shape
    heads = step_raw.shape[0]
    state = in_coeff.shape[1]
    model = out_proj.shape[1]
    chunks, pieces = channels // 256, model // 256
    width, piece = channels // chunks, model // pieces
    sub = width // 2
    padded = -(-heads // 8) * 8
    share = rows // n_head
    assert n_head == 4 and n_seq % 2 == 0 and rows <= 512
    vmem = pl.BlockSpec(memory_space=pltpu.VMEM)
    anywhere = pl.BlockSpec(memory_space=pl.ANY)
    dma = pltpu.SemaphoreType.DMA
    return pl.pallas_call(
        functools.partial(kernel, n_seq, n_head, heads, chunks, pieces),
        out_shape=pltpu.VMEM((share, model), BF16),
        in_specs=[anywhere] * 11,
        out_specs=vmem,
        scratch_shapes=[
            pltpu.VMEM(doc_starts.shape, doc_starts.dtype),
            pltpu.VMEM(step_raw.shape, F32),
            pltpu.VMEM((1, heads), F32),
            pltpu.VMEM((1, heads), F32),
            pltpu.VMEM((1, heads), F32),
            pltpu.VMEM(norm_gain.shape, F32),
            pltpu.VMEM(in_coeff.shape, BF16),
            pltpu.VMEM(out_coeff.shape, BF16),
            pltpu.VMEM((rows, channels), BF16),
            pltpu.VMEM((rows, channels), BF16),
            pltpu.VMEM((channels, model), BF16),
            pltpu.VMEM((padded, rows), F32),
            pltpu.VMEM((2 * padded, channels), BF16),
            pltpu.VMEM((2 * padded, rows), BF16),
            pltpu.VMEM((2 * padded, rows), BF16),
            pltpu.VMEM((rows, rows), BF16),
            pltpu.VMEM((rows, state), BF16),
            pltpu.VMEM((rows, channels), BF16),
            pltpu.VMEM((1, channels), F32),
            pltpu.VMEM((2, 2, 1, channels), F32),
            pltpu.VMEM((8, channels), F32),
            pltpu.VMEM((rows, channels), F32),
            pltpu.VMEM((rows, channels), F32),
            pltpu.VMEM((rows, 128), F32),
            pltpu.VMEM((rows, channels), BF16),
            pltpu.VMEM((chunks, 2, state, sub), BF16),
            pltpu.VMEM((2, 2, chunks, state, sub), BF16),
            pltpu.VMEM((chunks, 2, state, sub), BF16),
            pltpu.VMEM((2, chunks, 2, state, sub), BF16),
            pltpu.VMEM((chunks, 2, state, sub), BF16),
            pltpu.VMEM((n_head, 8, share), F32),
            pltpu.VMEM((n_head - 1, 8, share), F32),
            pltpu.VMEM((2 * pieces, 2 * share, piece), F32),
            pltpu.VMEM((2 * pieces, share, piece), BF16),
            pltpu.VMEM((2 * pieces, share, piece), BF16),
            pltpu.VMEM((pieces, share, piece), BF16),
            pltpu.VMEM((pieces, share, piece), BF16),
            dma((8,)),
            dma((3,)),
            pltpu.SemaphoreType.REGULAR,
            dma((2,)),
            dma((2, 2)),
            dma((2, chunks)),
            dma((2, 2, chunks)),
            dma((chunks, 2, 2)),
            dma((chunks, 2, 2)),
            dma((chunks, 2)),
            dma((n_head - 1, 2)),
            dma((2 * pieces, 2)),
            dma((pieces, 2)),
        ],
        compiler_params=pltpu.CompilerParams(
            collective_id=0, has_side_effects=True, vmem_limit_bytes=56 * 1024 * 1024
        ),
    )(
        doc_starts,
        step_raw,
        step_bias.reshape(1, -1),
        decay_rate.reshape(1, -1),
        skip_scale.reshape(1, -1),
        norm_gain,
        in_coeff,
        out_coeff,
        stream,
        gate_input,
        out_proj,
    )


def solution(mesh):
    in_specs = (
        P("seq", "head"),
        P("seq", "head"),
        P("seq", None),
        P("seq", None),
        P("head", "seq"),
        P("head"),
        P("head"),
        P("head"),
        P("head"),
        P("head", None),
        P(),
    )
    out_specs = P(("seq", "head"), None)
    body = functools.partial(local, mesh.shape["seq"], mesh.shape["head"])
    return jax.shard_map(body, mesh=mesh, in_specs=in_specs, out_specs=out_specs, check_vma=False)
```

```python
import functools

import jax
import jax.numpy as jnp
from jax import lax
from jax.experimental import pallas as pl
from jax.experimental.pallas import tpu as pltpu
from jax.sharding import PartitionSpec as P

EPSILON = 1e-05
F32 = jnp.float32
BF16 = jnp.bfloat16
MESH = pl.DeviceIdType.MESH
EARLY = 1
FAR_LAG = 2
LENT = (2, 1)


def dot(a, b, ca, cb):
    return lax.dot_general(a, b, (((ca,), (cb,)), ((), ())), preferred_element_type=F32)


def split(value, parts):
    pieces = []
    for _ in range(parts):
        piece = value.astype(BF16).astype(F32)
        pieces.append(piece)
        value = value - piece
    return jnp.concatenate(pieces, axis=0).astype(BF16)


def to_column(row):
    n = row.shape[1]
    eye = lax.broadcasted_iota(jnp.int32, (n, n), 0) == lax.broadcasted_iota(jnp.int32, (n, n), 1)
    return jnp.sum(jnp.where(eye, row, 0.0), axis=1, keepdims=True)


def lends(pair, last_pair):
    if last_pair + 1 < 2 * len(LENT):
        return 0 * pair
    return sum(jnp.where(pair == last_pair - i, count, 0) for i, count in enumerate(LENT))


def kernel(
    n_seq,
    n_head,
    heads,
    chunks,
    pieces,
    starts_hbm,
    step_hbm,
    bias_hbm,
    rate_hbm,
    skip_hbm,
    gain_hbm,
    in_hbm,
    out_hbm,
    stream_hbm,
    gate_hbm,
    proj_hbm,
    result_ref,
    starts_ref,
    step_ref,
    bias_ref,
    rate_ref,
    skip_ref,
    gain_ref,
    in_ref,
    out_ref,
    stream,
    gate,
    proj,
    pad,
    expand,
    factor_in,
    factor_out,
    pairs,
    carry_in,
    source,
    link_own,
    link_all,
    before_gate,
    base,
    slope,
    square,
    hidden,
    fresh_own,
    fresh_all,
    chain_out,
    states,
    incoming_all,
    square_out,
    square_in,
    held,
    near_out,
    near_in,
    far_out,
    far_in,
    relay_in,
    small_sem,
    load_sem,
    ready_sem,
    link_send,
    link_recv,
    fresh_send,
    fresh_recv,
    chain_send,
    chain_recv,
    return_send,
    return_recv,
    square_send,
    square_recv,
    near_send,
    near_recv,
    near_last,
    far_send,
    far_recv,
    relay_send,
    relay_recv,
):
    rows, channels = stream.shape
    state = in_ref.shape[1]
    width = channels // chunks
    head_size = channels // heads
    padded = pad.shape[0]
    sub = width // 2
    half = rows // 2
    share = rows // n_head
    piece = proj.shape[1] // pieces

    s = lax.axis_index("seq")
    g = lax.axis_index("head")
    parity = s % 2
    pair = s // 2
    last_pair = n_seq // 2 - 1
    core = g % 2
    side = g // 2
    near = side * 2 + (1 - core)
    far = (1 - side) * 2 + core
    cross = s + 1 - 2 * parity
    carrier = 2 * side + 1
    carries = core == 1
    helped = last_pair - pair
    lent = lends(pair, last_pair)
    borrowed = lends(helped, last_pair)
    helper = 2 * helped + parity
    peers = (near, far, (1 - side) * 2 + (1 - core))

    loads = [
        pltpu.make_async_copy(src, dst, load_sem.at[i])
        for i, (src, dst) in enumerate(((stream_hbm, stream), (gate_hbm, gate), (proj_hbm, proj)))
    ]
    smalls = [
        pltpu.make_async_copy(src, dst, small_sem.at[i])
        for i, (src, dst) in enumerate(
            (
                (step_hbm, step_ref),
                (bias_hbm, bias_ref),
                (rate_hbm, rate_ref),
                (starts_hbm, starts_ref),
                (in_hbm, in_ref),
                (skip_hbm, skip_ref),
                (gain_hbm, gain_ref),
                (out_hbm, out_ref),
            )
        )
    ]
    for small in smalls[:5]:
        small.start()
    loads[0].start()
    for small in smalls[5:]:
        small.start()

    barrier = pltpu.get_barrier_semaphore()
    for peer in peers:
        pl.semaphore_signal(barrier, inc=1, device_id=(s, peer), device_id_type=MESH)
    for peer in (g, near):
        pl.semaphore_signal(barrier, inc=1, device_id=(cross, peer), device_id_type=MESH)

    @pl.when(pair < last_pair)
    def _():
        pl.semaphore_signal(barrier, inc=1, device_id=(s + 2, g), device_id_type=MESH)

    @pl.when(borrowed > 0)
    def _():
        pl.semaphore_signal(barrier, inc=1, device_id=(helper, far), device_id_type=MESH)

    def remote(src, dst, send_sem, recv_sem, seq, head):
        return pltpu.make_async_remote_copy(
            src_ref=src,
            dst_ref=dst,
            send_sem=send_sem,
            recv_sem=recv_sem,
            device_id=(seq, head),
            device_id_type=MESH,
        )

    def slot(part, away):
        return 2 * part + 1 - away

    def link_copy(away):
        return remote(
            link_own,
            link_all.at[slot(core, away)],
            link_send.at[away],
            link_recv,
            cross if away else s,
            carrier,
        )

    def fresh_copy(k, away):
        return remote(
            fresh_own.at[k, 1 - parity if away else parity],
            fresh_all.at[k, slot(core, away)],
            fresh_send.at[away],
            fresh_recv.at[k],
            cross if away else s,
            carrier,
        )

    def chain_copy(k, part):
        return remote(
            chain_out.at[k, part],
            states.at[0, k, part],
            chain_send,
            chain_recv.at[k, part],
            (s + 2) % n_seq,
            g,
        )

    def return_copy(k, away, part, owner):
        return remote(
            states.at[1 - parity if away else parity, k, part],
            incoming_all.at[k, owner],
            return_send.at[away],
            return_recv.at[k, owner],
            cross if away else s,
            2 * side + part,
        )

    def arrived(dst, sem):
        remote(dst, dst, sem, sem, s, near).wait_recv()

    def left(src, sem):
        remote(src, src, sem, sem, s, near).wait_send()

    pad[...] = jnp.zeros_like(pad)
    for small in smalls[:3]:
        small.wait()
    raw = step_ref[...] + to_column(bias_ref[...])
    pad[pl.ds(0, heads), :] = jnp.maximum(raw, 0.0) + jnp.log(1.0 + jnp.exp(-jnp.abs(raw)))
    step_size = pad[...]
    head_row = lax.broadcasted_iota(jnp.int32, (padded, channels), 0) * head_size
    lane = lax.broadcasted_iota(jnp.int32, (padded, channels), 1)
    spread = jnp.where((lane >= head_row) & (lane < head_row + head_size), 1.0, 0.0)
    expand[...] = jnp.concatenate([spread, spread], axis=0).astype(BF16)
    rate = to_column(rate_ref[...])
    if padded > heads:
        rate = jnp.concatenate([rate, jnp.zeros((padded - heads, 1), F32)], axis=0)
    log_decay = -step_size * rate
    first = lax.broadcasted_iota(jnp.int32, (rows, rows), 0)
    second = lax.broadcasted_iota(jnp.int32, (rows, rows), 1)
    upper = jnp.where(first <= second, 1.0, 0.0).astype(BF16)
    sums = dot(split(log_decay, 3), upper, 1, 0)
    cumulative = sums[:padded] + sums[padded : 2 * padded] + sums[2 * padded :]
    middle = cumulative[:, half - 1 : half]
    last = cumulative[:, rows - 1 : rows]
    factor_in[...] = split(jnp.exp(middle - cumulative) * step_size, 2)

    for small in smalls[3:5]:
        small.wait()
    starts = starts_ref[...].astype(F32).reshape(1, -1)
    offset = s * rows
    place = (offset + lax.broadcasted_iota(jnp.int32, (rows, 1), 0)).astype(F32)
    place_lane = (offset + lax.broadcasted_iota(jnp.int32, (1, rows), 1)).astype(F32)
    doc = jnp.sum(jnp.where(starts <= place, 1.0, 0.0), axis=1, keepdims=True)
    before = jnp.sum(jnp.where(starts <= (offset - 1).astype(F32), 1.0, 0.0), axis=1, keepdims=True)
    doc_end = doc[rows - 1 : rows, :]
    joined_end = jnp.where(doc_end == before, 1.0, 0.0)

    def per_channel(column):
        return jnp.sum(spread * column, axis=0, keepdims=True)

    link_own[...] = per_channel(jnp.exp(last)) * joined_end
    end_gate = per_channel(jnp.exp(last - middle))
    before_gate[1:2, :] = end_gate
    in_end = jnp.where(doc == doc_end, in_ref[...].astype(F32), 0.0).astype(BF16)

    greetings = len(peers) + 2 + (pair > 0).astype(jnp.int32) + (lent > 0).astype(jnp.int32)
    pl.semaphore_wait(barrier, greetings)

    @pl.when(carries & (pair > 0))
    def _():
        pl.semaphore_signal(ready_sem, inc=1, device_id=(s - 2, g), device_id_type=MESH)

    link_copy(1).start()

    @pl.when(core == 0)
    def _():
        link_copy(0).start()

    @pl.when(carries)
    def _():
        link_all[3] = link_own[...]

    loads[0].wait()
    loads[1].start()
    loads[2].start()

    def columns(k):
        return pl.ds(pl.multiple_of(k * width, width), width)

    def make_summary(k, _):
        cols = columns(k)
        scale = dot(factor_in[...], expand[:, cols], 0, 0)
        scaled = (stream[:, cols].astype(F32) * scale).astype(BF16)
        source[:, cols] = scaled
        fresh = dot(in_end, scaled, 0, 0) * before_gate[1:2, cols]

        for i in range(2):
            fresh_own[k, i] = fresh[:, i * sub : (i + 1) * sub].astype(BF16)
        fresh_copy(k, 1).start()

        @pl.when(core == 0)
        def _():
            fresh_copy(k, 0).start()

        @pl.when(carries)
        def _():
            fresh_all[k, 3] = fresh_own[k, parity]

        return 0

    lax.fori_loop(0, chunks, make_summary, 0)

    for small in smalls[5:]:
        small.wait()

    factor_out[...] = split(jnp.exp(cumulative - middle), 2)
    before_gate[3:4, :] = gain_ref[...].reshape(1, -1)
    doc_lane = jnp.sum(jnp.where(to_column(starts) <= place_lane, 1.0, 0.0), axis=0, keepdims=True)
    before_gate[0:1, :] = per_channel(jnp.exp(middle))
    skip = to_column(skip_ref[...])
    if padded > heads:
        skip = jnp.concatenate([skip, jnp.zeros((padded - heads, 1), F32)], axis=0)
    before_gate[2:3, :] = per_channel(skip)
    carry_in[...] = jnp.where(doc == before, out_ref[...].astype(F32), 0.0).astype(BF16)
    scores = dot(out_ref[...], in_ref[...], 1, 1)
    live = (first >= second) & (doc == doc_lane)
    pairs[...] = jnp.where(live, scores, 0.0).astype(BF16)
    square[...] = jnp.zeros_like(square)
    loads[1].wait()

    @pl.when(s == 0)
    def _():
        incoming_all[...] = jnp.zeros_like(incoming_all)

    @pl.when(carries)
    def _():
        arrived(link_all.at[pl.ds(0, 3)], link_recv)

    def local_part(k):
        cols = columns(k)
        gate_value = gate[:, cols].astype(F32)
        silu = gate_value * (0.5 * jnp.tanh(0.5 * gate_value) + 0.5)
        within = jnp.concatenate(
            [
                dot(pairs[:half, :half], source[:half, cols], 1, 0),
                dot(pairs[half:, :], source[:, cols], 1, 0),
            ],
            axis=0,
        )
        factor = dot(factor_out[...], expand[:, cols], 0, 0) * silu
        slope[:, cols] = factor
        base[:, cols] = within * factor + stream[:, cols].astype(F32) * before_gate[2:3, cols] * silu

    def chain_step(k):
        cols = pl.ds(pl.multiple_of(k * width + parity * sub, sub), sub)
        arrived(fresh_all.at[k, pl.ds(0, 3)], fresh_recv.at[k])

        for part in range(2):
            even, odd = 2 * part + 1 - parity, 2 * part + parity
            keep_even, keep_odd = link_all[even, :, cols], link_all[odd, :, cols]
            fresh_even = fresh_all[k, even].astype(F32)
            fresh_odd = fresh_all[k, odd].astype(F32)

            @pl.when(pair > 0)
            def _():
                chain_copy(k, part).wait_recv()
                between = keep_even * states[0, k, part].astype(F32) + fresh_even
                states[1, k, part] = between.astype(BF16)
                chain_out[k, part] = (keep_odd * between + fresh_odd).astype(BF16)

            @pl.when(pair == 0)
            def _():
                states[1, k, part] = fresh_all[k, even]
                chain_out[k, part] = (keep_odd * fresh_even + fresh_odd).astype(BF16)

            @pl.when(pair < last_pair)
            def _():
                chain_copy(k, part).start()

            @pl.when(cross > 0)
            def _():
                return_copy(k, 1, part, parity).start()

            @pl.when(s > 0)
            def _():
                if part == 0:
                    return_copy(k, 0, part, parity).start()
                else:
                    incoming_all[k, parity] = states[parity, k, part]

    def finish(k):
        @pl.when(s > 0)
        def _():
            return_copy(k, 1, core, 1 - parity).wait_recv()

            @pl.when(core == 0)
            def _():
                return_copy(k, 0, core, parity).wait_recv()

        cols = columns(k)
        incoming = jnp.concatenate([incoming_all[k, i].astype(F32) for i in range(2)], axis=1)
        incoming = (incoming * before_gate[0:1, cols]).astype(BF16)
        carried = dot(carry_in[...], incoming, 1, 0)
        gated = base[:, cols] + slope[:, cols] * carried
        hidden[:, cols] = (gated * before_gate[3:4, cols]).astype(BF16)
        squares = gated * gated
        total = square[...]
        for i in range(width // 128):
            total = total + squares[:, i * 128 : (i + 1) * 128]
        square[...] = total

    lead = jnp.where(carries & (pair < EARLY), 0, chunks)

    def main_step(step, _):
        @pl.when(carries & (step >= lead) & (step < lead + chunks))
        def _():
            chain_step(step - lead)

        @pl.when(step < chunks)
        def _():
            local_part(step)

        return 0

    @pl.when(carries & (pair < last_pair))
    def _():
        pl.semaphore_wait(ready_sem, 1)

    lax.fori_loop(0, chunks + jnp.where(carries, lead, 0), main_step, 0)

    def finish_step(k, _):
        finish(k)
        return 0

    lax.fori_loop(0, chunks, finish_step, 0)

    loads[2].wait()

    def piece_columns(j):
        return pl.ds(pl.multiple_of(j * piece, piece), piece)

    def near_copy(stage, j, sem):
        at = stage * pieces + j
        return remote(near_out.at[at], near_in.at[at], near_send, sem, s, near)

    def far_copy(j):
        return remote(far_out.at[j], far_in.at[j], far_send, far_recv.at[j], s, far)

    def lend_copy(j):
        return remote(
            far_out.at[j], relay_in.at[j - 1], far_send, relay_recv.at[j - 1], helper, far
        )

    def relay_copy(i):
        return remote(
            relay_in.at[i], far_in.at[i + 1], relay_send.at[i], far_recv.at[i + 1], helper, g
        )

    def half_rows(which):
        return pl.ds(pl.multiple_of(which * 2 * share, 2 * share), 2 * share)

    def core_rows(which):
        return pl.ds(pl.multiple_of(which * share, share), share)

    def project(stage, which, j):
        held[stage * pieces + j] = dot(hidden[half_rows(which), :], proj[:, piece_columns(j)], 1, 0)
        near_out[stage * pieces + j] = held[stage * pieces + j, core_rows(1 - core), :].astype(BF16)
        near_copy(stage, j, near_recv.at[j] if stage == 0 else near_last).start()

    def pass_on(j):
        near_copy(0, j, near_recv.at[j]).wait_recv()
        both = held[j, core_rows(core), :] + near_in[j].astype(F32)
        far_out[j] = both.astype(BF16)
        lend = (j >= 1) & (j <= lent)

        @pl.when(lend)
        def _():
            lend_copy(j).start()

        @pl.when(jnp.logical_not(lend))
        def _():
            far_copy(j).start()

    def square_copy(i):
        return remote(
            square_out.at[peers[i]], square_in.at[i], square_send, square_recv, s, peers[i]
        )

    def send_squares():
        for owner in range(n_head):
            block = square[owner * share : (owner + 1) * share, :]
            sums_lane = jnp.sum(block.T, axis=0, keepdims=True)
            square_out[owner] = jnp.broadcast_to(sums_lane, (8, share))
        for i in range(len(peers)):
            square_copy(i).start()

    def far_step(j, _):
        @pl.when(j < pieces)
        def _():
            project(0, 1 - side, j)

        @pl.when(j >= FAR_LAG)
        def _():
            pass_on(j - FAR_LAG)

        @pl.when(j == FAR_LAG)
        def _():
            send_squares()

        return 0

    lax.fori_loop(0, pieces + FAR_LAG, far_step, 0)

    def near_step(j, _):
        project(1, side, j)
        return 0

    lax.fori_loop(0, pieces, near_step, 0)

    def relay_step(i, _):
        @pl.when(i < borrowed)
        def _():
            remote(
                far_out.at[i + 1], relay_in.at[i], far_send, relay_recv.at[i], helper, far
            ).wait_recv()
            relay_copy(i).start()

        return 0

    lax.fori_loop(0, LENT[0], relay_step, 0)

    arrived(square_in, square_recv)
    total = square_out[g]
    for i in range(len(peers)):
        total = total + square_in[i]
    mean = jnp.broadcast_to(total[0:1, :], (128, share)).T / (channels * n_head)
    scale_row = lax.rsqrt(mean + EPSILON)[:, 0:1]

    arrived(near_in.at[pl.ds(pieces, pieces)], near_last)

    def collect(j, _):
        far_copy(j).wait_recv()
        at = pieces + j
        whole = held[at, core_rows(core), :] + near_in[at].astype(F32) + far_in[j].astype(F32)
        result_ref[:, piece_columns(j)] = (whole * scale_row).astype(BF16)
        return 0

    lax.fori_loop(0, pieces, collect, 0)

    link_copy(1).wait_send()
    left(fresh_own.at[:, 0], fresh_send.at[1])

    @pl.when(core == 0)
    def _():
        link_copy(0).wait_send()
        left(fresh_own.at[:, 0], fresh_send.at[0])

    @pl.when(carries & (pair < last_pair))
    def _():
        left(chain_out, chain_send)

    @pl.when(carries & (cross > 0))
    def _():
        left(states.at[0], return_send.at[1])

    @pl.when(carries & (s > 0))
    def _():
        left(states.at[0, :, 0], return_send.at[0])

    left(square_out.at[pl.ds(0, 3)], square_send)
    left(near_out, near_send)
    left(far_out, far_send)

    def drain_relay(i, _):
        @pl.when(i < borrowed)
        def _():
            relay_copy(i).wait_send()

        return 0

    lax.fori_loop(0, LENT[0], drain_relay, 0)


def local(
    n_seq,
    n_head,
    stream,
    gate_input,
    in_coeff,
    out_coeff,
    step_raw,
    step_bias,
    decay_rate,
    skip_scale,
    norm_gain,
    out_proj,
    doc_starts,
):
    rows, channels = stream.shape
    heads = step_raw.shape[0]
    state = in_coeff.shape[1]
    model = out_proj.shape[1]
    chunks, pieces = channels // 256, model // 256
    width, piece = channels // chunks, model // pieces
    sub = width // 2
    padded = -(-heads // 8) * 8
    share = rows // n_head
    assert n_head == 4 and n_seq % 2 == 0 and rows <= 512
    vmem = pl.BlockSpec(memory_space=pltpu.VMEM)
    anywhere = pl.BlockSpec(memory_space=pl.ANY)
    dma = pltpu.SemaphoreType.DMA
    return pl.pallas_call(
        functools.partial(kernel, n_seq, n_head, heads, chunks, pieces),
        out_shape=pltpu.VMEM((share, model), BF16),
        in_specs=[anywhere] * 11,
        out_specs=vmem,
        scratch_shapes=[
            pltpu.VMEM(doc_starts.shape, doc_starts.dtype),
            pltpu.VMEM(step_raw.shape, F32),
            pltpu.VMEM((1, heads), F32),
            pltpu.VMEM((1, heads), F32),
            pltpu.VMEM((1, heads), F32),
            pltpu.VMEM(norm_gain.shape, F32),
            pltpu.VMEM(in_coeff.shape, BF16),
            pltpu.VMEM(out_coeff.shape, BF16),
            pltpu.VMEM((rows, channels), BF16),
            pltpu.VMEM((rows, channels), BF16),
            pltpu.VMEM((channels, model), BF16),
            pltpu.VMEM((padded, rows), F32),
            pltpu.VMEM((2 * padded, channels), BF16),
            pltpu.VMEM((2 * padded, rows), BF16),
            pltpu.VMEM((2 * padded, rows), BF16),
            pltpu.VMEM((rows, rows), BF16),
            pltpu.VMEM((rows, state), BF16),
            pltpu.VMEM((rows, channels), BF16),
            pltpu.VMEM((1, channels), F32),
            pltpu.VMEM((4, 1, channels), F32),
            pltpu.VMEM((8, channels), F32),
            pltpu.VMEM((rows, channels), F32),
            pltpu.VMEM((rows, channels), F32),
            pltpu.VMEM((rows, 128), F32),
            pltpu.VMEM((rows, channels), BF16),
            pltpu.VMEM((chunks, 2, state, sub), BF16),
            pltpu.VMEM((chunks, 4, state, sub), BF16),
            pltpu.VMEM((chunks, 2, state, sub), BF16),
            pltpu.VMEM((2, chunks, 2, state, sub), BF16),
            pltpu.VMEM((chunks, 2, state, sub), BF16),
            pltpu.VMEM((n_head, 8, share), F32),
            pltpu.VMEM((n_head - 1, 8, share), F32),
            pltpu.VMEM((2 * pieces, 2 * share, piece), F32),
            pltpu.VMEM((2 * pieces, share, piece), BF16),
            pltpu.VMEM((2 * pieces, share, piece), BF16),
            pltpu.VMEM((pieces, share, piece), BF16),
            pltpu.VMEM((pieces, share, piece), BF16),
            pltpu.VMEM((LENT[0], share, piece), BF16),
            dma((8,)),
            dma((3,)),
            pltpu.SemaphoreType.REGULAR,
            dma((2,)),
            dma,
            dma((2,)),
            dma((chunks,)),
            dma,
            dma((chunks, 2)),
            dma((2,)),
            dma((chunks, 2)),
            dma,
            dma,
            dma,
            dma((pieces,)),
            dma,
            dma,
            dma((pieces,)),
            dma((LENT[0],)),
            dma((LENT[0],)),
        ],
        compiler_params=pltpu.CompilerParams(
            collective_id=0, has_side_effects=True, vmem_limit_bytes=56 * 1024 * 1024
        ),
    )(
        doc_starts,
        step_raw,
        step_bias.reshape(1, -1),
        decay_rate.reshape(1, -1),
        skip_scale.reshape(1, -1),
        norm_gain,
        in_coeff,
        out_coeff,
        stream,
        gate_input,
        out_proj,
    )


def solution(mesh):
    in_specs = (
        P("seq", "head"),
        P("seq", "head"),
        P("seq", None),
        P("seq", None),
        P("head", "seq"),
        P("head"),
        P("head"),
        P("head"),
        P("head"),
        P("head", None),
        P(),
    )
    out_specs = P(("seq", "head"), None)
    body = functools.partial(local, mesh.shape["seq"], mesh.shape["head"])
    return jax.shard_map(body, mesh=mesh, in_specs=in_specs, out_specs=out_specs, check_vma=False)
```

```python
import functools

import jax
import jax.numpy as jnp
from jax import lax
from jax.experimental import pallas as pl
from jax.experimental.pallas import tpu as pltpu
from jax.sharding import PartitionSpec as P

EPSILON = 1e-05
F32 = jnp.float32
BF16 = jnp.bfloat16
MESH = pl.DeviceIdType.MESH
LEAD = 1
LEND_FROM = 2
FAR_LAG = 2
READY = 2
SOON = 1
LAG = 3
LENT = ((2, 2), (1, 0))
SLOTS = max(max(counts) for counts in LENT)


def dot(a, b, ca, cb):
    return lax.dot_general(a, b, (((ca,), (cb,)), ((), ())), preferred_element_type=F32)


def split(value, parts):
    pieces = []
    for _ in range(parts):
        piece = value.astype(BF16).astype(F32)
        pieces.append(piece)
        value = value - piece
    return jnp.concatenate(pieces, axis=0).astype(BF16)


def to_column(row):
    n = row.shape[1]
    eye = lax.broadcasted_iota(jnp.int32, (n, n), 0) == lax.broadcasted_iota(jnp.int32, (n, n), 1)
    return jnp.sum(jnp.where(eye, row, 0.0), axis=1, keepdims=True)


def lends(pair, last_pair, core):
    if last_pair + 1 < 2 * len(LENT):
        return 0 * pair
    return sum(
        jnp.where(pair == last_pair - i, jnp.where(core == 0, *counts), 0)
        for i, counts in enumerate(LENT)
    )


def kernel(
    n_seq,
    n_head,
    heads,
    chunks,
    pieces,
    starts_hbm,
    step_hbm,
    bias_hbm,
    rate_hbm,
    skip_hbm,
    gain_hbm,
    in_hbm,
    out_hbm,
    stream_hbm,
    gate_hbm,
    proj_hbm,
    result_ref,
    starts_ref,
    step_ref,
    bias_ref,
    rate_ref,
    skip_ref,
    gain_ref,
    in_ref,
    out_ref,
    stream,
    gate,
    proj,
    pad,
    expand,
    factor_in,
    factor_out,
    pairs,
    carry_in,
    source,
    link_own,
    link_all,
    before_gate,
    base,
    slope,
    square,
    hidden,
    fresh_own,
    fresh_all,
    chain_out,
    states,
    incoming_all,
    square_out,
    square_in,
    held,
    near_out,
    near_in,
    far_out,
    far_in,
    relay_in,
    extra_out,
    extra_in,
    small_sem,
    load_sem,
    ready_sem,
    link_send,
    link_recv,
    fresh_send,
    fresh_recv,
    chain_send,
    chain_recv,
    return_send,
    return_recv,
    square_send,
    square_recv,
    near_send,
    near_recv,
    near_last,
    far_send,
    far_recv,
    relay_send,
    relay_recv,
    extra_send,
    extra_recv,
):
    rows, channels = stream.shape
    state = in_ref.shape[1]
    width = channels // chunks
    head_size = channels // heads
    padded = pad.shape[0]
    sub = width // 2
    half = rows // 2
    share = rows // n_head
    piece = proj.shape[1] // pieces

    s = lax.axis_index("seq")
    g = lax.axis_index("head")
    parity = s % 2
    pair = s // 2
    last_pair = n_seq // 2 - 1
    core = g % 2
    side = g // 2
    near = side * 2 + (1 - core)
    far = (1 - side) * 2 + core
    cross = s + 1 - 2 * parity
    carrier = 2 * side + 1
    carries = core == 1
    helped = last_pair - pair
    lent = lends(pair, last_pair, core)
    borrowed = lends(helped, last_pair, core)
    helper = 2 * helped + parity
    peers = (near, far, (1 - side) * 2 + (1 - core))

    loads = [
        pltpu.make_async_copy(src, dst, load_sem.at[i])
        for i, (src, dst) in enumerate(((stream_hbm, stream), (gate_hbm, gate), (proj_hbm, proj)))
    ]
    smalls = [
        pltpu.make_async_copy(src, dst, small_sem.at[i])
        for i, (src, dst) in enumerate(
            (
                (step_hbm, step_ref),
                (bias_hbm, bias_ref),
                (rate_hbm, rate_ref),
                (starts_hbm, starts_ref),
                (in_hbm, in_ref),
                (skip_hbm, skip_ref),
                (gain_hbm, gain_ref),
                (out_hbm, out_ref),
            )
        )
    ]
    for small in smalls[:5]:
        small.start()
    loads[0].start()
    for small in smalls[5:]:
        small.start()

    barrier = pltpu.get_barrier_semaphore()
    for peer in peers:
        pl.semaphore_signal(barrier, inc=1, device_id=(s, peer), device_id_type=MESH)
    for peer in (g, near):
        pl.semaphore_signal(barrier, inc=1, device_id=(cross, peer), device_id_type=MESH)

    @pl.when(pair < last_pair)
    def _():
        pl.semaphore_signal(barrier, inc=1, device_id=(s + 2, g), device_id_type=MESH)

    @pl.when(borrowed > 0)
    def _():
        pl.semaphore_signal(barrier, inc=1, device_id=(helper, far), device_id_type=MESH)

    def remote(src, dst, send_sem, recv_sem, seq, head):
        return pltpu.make_async_remote_copy(
            src_ref=src,
            dst_ref=dst,
            send_sem=send_sem,
            recv_sem=recv_sem,
            device_id=(seq, head),
            device_id_type=MESH,
        )

    def slot(part, away):
        return 2 * part + 1 - away

    def link_copy(away):
        return remote(
            link_own,
            link_all.at[slot(core, away)],
            link_send.at[away],
            link_recv,
            cross if away else s,
            carrier,
        )

    def fresh_copy(k, away):
        return remote(
            fresh_own.at[k, 1 - parity if away else parity],
            fresh_all.at[k, slot(core, away)],
            fresh_send.at[away],
            fresh_recv.at[k],
            cross if away else s,
            carrier,
        )

    def chain_copy(k, part):
        return remote(
            chain_out.at[k, part],
            states.at[0, k, part],
            chain_send,
            chain_recv.at[k, part],
            (s + 2) % n_seq,
            g,
        )

    def return_copy(k, away, part, owner):
        return remote(
            states.at[1 - parity if away else parity, k, part],
            incoming_all.at[k, owner],
            return_send.at[away],
            return_recv.at[k],
            cross if away else s,
            2 * side + part,
        )

    def arrived(dst, sem):
        remote(dst, dst, sem, sem, s, near).wait_recv()

    def left(src, sem):
        remote(src, src, sem, sem, s, near).wait_send()

    pad[...] = jnp.zeros_like(pad)
    head_row = lax.broadcasted_iota(jnp.int32, (padded, channels), 0) * head_size
    lane = lax.broadcasted_iota(jnp.int32, (padded, channels), 1)
    spread = jnp.where((lane >= head_row) & (lane < head_row + head_size), 1.0, 0.0)
    expand[...] = jnp.concatenate([spread, spread], axis=0).astype(BF16)
    first = lax.broadcasted_iota(jnp.int32, (rows, rows), 0)
    second = lax.broadcasted_iota(jnp.int32, (rows, rows), 1)
    upper = jnp.where(first <= second, 1.0, 0.0).astype(BF16)
    pairs[...] = upper
    for small in smalls[:3]:
        small.wait()
    raw = step_ref[...] + to_column(bias_ref[...])
    pad[pl.ds(0, heads), :] = jnp.maximum(raw, 0.0) + jnp.log(1.0 + jnp.exp(-jnp.abs(raw)))
    step_size = pad[...]
    rate = to_column(rate_ref[...])
    if padded > heads:
        rate = jnp.concatenate([rate, jnp.zeros((padded - heads, 1), F32)], axis=0)
    log_decay = -step_size * rate
    sums = dot(split(log_decay, 3), pairs[...], 1, 0)
    cumulative = sums[:padded] + sums[padded : 2 * padded] + sums[2 * padded :]
    middle = cumulative[:, half - 1 : half]
    last = cumulative[:, rows - 1 : rows]
    factor_in[...] = split(jnp.exp(middle - cumulative) * step_size, 2)

    for small in smalls[3:5]:
        small.wait()
    starts = starts_ref[...].astype(F32).reshape(1, -1)
    offset = s * rows
    place = (offset + lax.broadcasted_iota(jnp.int32, (rows, 1), 0)).astype(F32)
    place_lane = (offset + lax.broadcasted_iota(jnp.int32, (1, rows), 1)).astype(F32)
    doc = jnp.sum(jnp.where(starts <= place, 1.0, 0.0), axis=1, keepdims=True)
    before = jnp.sum(jnp.where(starts <= (offset - 1).astype(F32), 1.0, 0.0), axis=1, keepdims=True)
    doc_end = doc[rows - 1 : rows, :]
    joined_end = jnp.where(doc_end == before, 1.0, 0.0)

    def per_channel(column):
        return jnp.sum(spread * column, axis=0, keepdims=True)

    link_own[...] = per_channel(jnp.exp(last)) * joined_end
    end_gate = per_channel(jnp.exp(last - middle))
    before_gate[1:2, :] = end_gate
    in_end = jnp.where(doc == doc_end, in_ref[...].astype(F32), 0.0).astype(BF16)

    loads[0].wait()
    loads[1].start()
    loads[2].start()

    def columns(k):
        return pl.ds(pl.multiple_of(k * width, width), width)

    def meet():
        greetings = len(peers) + 2 + (pair > 0).astype(jnp.int32) + (lent > 0).astype(jnp.int32)
        pl.semaphore_wait(barrier, greetings)

        @pl.when(carries & (pair > 0))
        def _():
            pl.semaphore_signal(ready_sem, inc=1, device_id=(s - 2, g), device_id_type=MESH)

        link_copy(1).start()

        @pl.when(core == 0)
        def _():
            link_copy(0).start()

        @pl.when(carries)
        def _():
            link_all[3] = link_own[...]

    def make_summary(k, _):
        cols = columns(k)
        scale = dot(factor_in[...], expand[:, cols], 0, 0)
        scaled = (stream[:, cols].astype(F32) * scale).astype(BF16)
        source[:, cols] = scaled
        fresh = dot(in_end, scaled, 0, 0) * before_gate[1:2, cols]

        for i in range(2):
            fresh_own[k, i] = fresh[:, i * sub : (i + 1) * sub].astype(BF16)
        @pl.when(k == 0)
        def _():
            meet()

        fresh_copy(k, 1).start()

        @pl.when(core == 0)
        def _():
            fresh_copy(k, 0).start()

        @pl.when(carries)
        def _():
            fresh_all[k, 3] = fresh_own[k, parity]

        return 0

    lax.fori_loop(0, chunks, make_summary, 0)

    for small in smalls[5:]:
        small.wait()

    factor_out[...] = split(jnp.exp(cumulative - middle), 2)
    before_gate[3:4, :] = gain_ref[...].reshape(1, -1)
    doc_lane = jnp.sum(jnp.where(to_column(starts) <= place_lane, 1.0, 0.0), axis=0, keepdims=True)
    before_gate[0:1, :] = per_channel(jnp.exp(middle))
    skip = to_column(skip_ref[...])
    if padded > heads:
        skip = jnp.concatenate([skip, jnp.zeros((padded - heads, 1), F32)], axis=0)
    before_gate[2:3, :] = per_channel(skip)
    carry_in[...] = jnp.where(doc == before, out_ref[...].astype(F32), 0.0).astype(BF16)
    scores = dot(out_ref[...], in_ref[...], 1, 1)
    live = (first >= second) & (doc == doc_lane)
    pairs[...] = jnp.where(live, scores, 0.0).astype(BF16)
    square[...] = jnp.zeros_like(square)
    loads[1].wait()

    @pl.when(s == 0)
    def _():
        incoming_all[...] = jnp.zeros_like(incoming_all)

    @pl.when(carries)
    def _():
        arrived(link_all.at[pl.ds(0, 3)], link_recv)

    def local_part(k):
        cols = columns(k)
        gate_value = gate[:, cols].astype(F32)
        silu = gate_value * (0.5 * jnp.tanh(0.5 * gate_value) + 0.5)
        within = jnp.concatenate(
            [
                dot(pairs[:half, :half], source[:half, cols], 1, 0),
                dot(pairs[half:, :], source[:, cols], 1, 0),
            ],
            axis=0,
        )
        factor = dot(factor_out[...], expand[:, cols], 0, 0) * silu
        slope[:, cols] = factor
        base[:, cols] = within * factor + stream[:, cols].astype(F32) * before_gate[2:3, cols] * silu

    def chain_step(k):
        cols = pl.ds(pl.multiple_of(k * width + parity * sub, sub), sub)
        arrived(fresh_all.at[k, pl.ds(0, 3)], fresh_recv.at[k])

        for part in range(2):
            even, odd = 2 * part + 1 - parity, 2 * part + parity
            keep_even, keep_odd = link_all[even, :, cols], link_all[odd, :, cols]
            fresh_even = fresh_all[k, even].astype(F32)
            fresh_odd = fresh_all[k, odd].astype(F32)

            @pl.when(pair > 0)
            def _():
                chain_copy(k, part).wait_recv()
                between = keep_even * states[0, k, part].astype(F32) + fresh_even
                states[1, k, part] = between.astype(BF16)
                chain_out[k, part] = (keep_odd * between + fresh_odd).astype(BF16)

            @pl.when(pair == 0)
            def _():
                states[1, k, part] = fresh_all[k, even]
                chain_out[k, part] = (keep_odd * fresh_even + fresh_odd).astype(BF16)

            @pl.when(pair < last_pair)
            def _():
                chain_copy(k, part).start()

            @pl.when(cross > 0)
            def _():
                return_copy(k, 1, part, parity).start()

            @pl.when(s > 0)
            def _():
                if part == 0:
                    return_copy(k, 0, part, parity).start()
                else:
                    incoming_all[k, parity] = states[parity, k, part]

    def take(k):
        @pl.when(carries & (s > 0))
        def _():
            arrived(incoming_all.at[k, 0], return_recv.at[k])

        @pl.when((core == 0) & (s > 0))
        def _():
            arrived(incoming_all.at[k], return_recv.at[k])

    def half_rows(which):
        return pl.ds(pl.multiple_of(which * half, half), half)

    def piece_columns(j):
        return pl.ds(pl.multiple_of(j * piece, piece), piece)

    def finish(k, span):
        cols = columns(k)
        incoming = jnp.concatenate([incoming_all[k, i].astype(F32) for i in range(2)], axis=1)
        incoming = (incoming * before_gate[0:1, cols]).astype(BF16)
        carried = dot(carry_in[span, :], incoming, 1, 0)
        gated = base[span, cols] + slope[span, cols] * carried
        hidden[span, cols] = (gated * before_gate[3:4, cols]).astype(BF16)
        squares = gated * gated
        total = square[span, :]
        for i in range(width // 128):
            total = total + squares[:, i * 128 : (i + 1) * 128]
        square[span, :] = total

    def product(span, depth, j):
        return dot(hidden[span, depth], proj[depth, piece_columns(j)], 1, 0)

    early_depth = pl.ds(0, channels - width)
    late_depth = pl.ds(channels - width, width)

    lead = jnp.where(pair == 0, LEAD, chunks)


    def main_step(step, _):
        @pl.when(carries & (step >= lead) & (step < lead + chunks))
        def _():
            chain_step(step - lead)

        @pl.when(step < chunks)
        def _():
            local_part(step)

        @pl.when(carries & (step >= lead + LAG))
        def _():
            take(step - lead - LAG)
            finish(step - lead - LAG, pl.ds(0, rows))

        return 0

    @pl.when(carries & (pair < last_pair))
    def _():
        pl.semaphore_wait(ready_sem, 1)

    lax.fori_loop(0, chunks + jnp.where(carries, lead, 0), main_step, 0)

    loads[2].wait()

    def finish_step(k, _):
        take(k)
        finish(k, pl.ds(0, rows))
        return 0

    lax.fori_loop(jnp.where(carries, chunks - LAG, 0), chunks - 1, finish_step, 0)
    for j in range(READY):
        held[j] = product(half_rows(1 - side), early_depth, j)
    take(chunks - 1)
    finish(chunks - 1, half_rows(1 - side))

    def near_copy(stage, j, sem):
        at = stage * pieces + j
        return remote(near_out.at[at], near_in.at[at], near_send, sem, s, near)

    def far_copy(j):
        return remote(far_out.at[j], far_in.at[j], far_send, far_recv.at[j], s, far)

    def lend_copy(j):
        return remote(
            far_out.at[j],
            relay_in.at[j - LEND_FROM],
            far_send,
            relay_recv.at[j - LEND_FROM],
            helper,
            far,
        )

    def relay_copy(i):
        return remote(
            relay_in.at[i],
            far_in.at[i + LEND_FROM],
            relay_send.at[i],
            far_recv.at[i + LEND_FROM],
            helper,
            g,
        )

    def core_rows(which):
        return pl.ds(pl.multiple_of(which * share, share), share)

    def extra_copy():
        return remote(extra_out, extra_in, extra_send, extra_recv, s, near)

    def extra_far_copy():
        return remote(
            extra_out, far_in.at[pieces - 1], extra_send, far_recv.at[pieces - 1], s, 2 * (1 - side)
        )

    def exchange(stage, j):
        at = stage * pieces + j
        near_out[at] = held[at, core_rows(1 - core), :].astype(BF16)
        near_copy(stage, j, near_recv.at[j] if stage == 0 else near_last).start()

    def project(stage, which, j):
        at = stage * pieces + j
        held[at] = product(half_rows(which), pl.ds(0, channels), j)

    def pass_on(j):
        near_copy(0, j, near_recv.at[j]).wait_recv()
        both = held[j, core_rows(core), :] + near_in[j].astype(F32)
        far_out[j] = both.astype(BF16)
        lend = (j >= LEND_FROM) & (j < LEND_FROM + lent)

        @pl.when(lend)
        def _():
            lend_copy(j).start()

        @pl.when(jnp.logical_not(lend))
        def _():
            far_copy(j).start()

    def pass_on_extra():
        extra_copy().wait_recv()
        both = held[pieces - 1, core_rows(1 - core), :] + extra_in[...].astype(F32)
        extra_out[...] = both.astype(BF16)
        extra_far_copy().start()

    def square_copy(i):
        return remote(
            square_out.at[peers[i]], square_in.at[i], square_send, square_recv, s, peers[i]
        )

    def send_squares():
        for owner in range(n_head):
            block = square[owner * share : (owner + 1) * share, :]
            sums_lane = jnp.sum(block.T, axis=0, keepdims=True)
            square_out[owner] = jnp.broadcast_to(sums_lane, (8, share))
        for i in range(len(peers)):
            square_copy(i).start()

    def far_step(j, _):
        @pl.when(j < READY)
        def _():
            held[j] = held[j] + product(half_rows(1 - side), late_depth, j)

        @pl.when((j >= READY) & (j < pieces))
        def _():
            project(0, 1 - side, j)

        @pl.when((j < pieces - 1) | ((j == pieces - 1) & (core == 0)))
        def _():
            exchange(0, j)

        @pl.when((j == pieces - 1) & (core == 0))
        def _():
            extra_out[...] = held[pieces - 1, core_rows(core), :].astype(BF16)
            extra_copy().start()

        @pl.when(j == SOON)
        def _():
            pass_on(0)
            finish(chunks - 1, half_rows(side))
            send_squares()

        @pl.when(carries & (j == pieces + FAR_LAG - 1))
        def _():
            pass_on_extra()

        @pl.when((j > FAR_LAG) & (carries | (j < pieces + FAR_LAG - 1)))
        def _():
            pass_on(j - FAR_LAG)

        return 0

    lax.fori_loop(0, pieces + FAR_LAG, far_step, 0)

    def near_step(j, _):
        project(1, side, j)
        exchange(1, j)
        return 0

    lax.fori_loop(0, pieces, near_step, 0)

    def relay_step(i, _):
        @pl.when(i < borrowed)
        def _():
            remote(
                far_out.at[i], relay_in.at[i], far_send, relay_recv.at[i], helper, far
            ).wait_recv()
            relay_copy(i).start()

        return 0

    lax.fori_loop(0, SLOTS, relay_step, 0)

    arrived(square_in, square_recv)
    total = square_out[g]
    for i in range(len(peers)):
        total = total + square_in[i]
    mean = jnp.broadcast_to(total[0:1, :], (128, share)).T / (channels * n_head)
    scale_row = lax.rsqrt(mean + EPSILON)[:, 0:1]

    arrived(near_in.at[pl.ds(pieces, pieces)], near_last)

    def collect(j, _):
        far_copy(j).wait_recv()
        at = pieces + j
        whole = held[at, core_rows(core), :] + near_in[at].astype(F32) + far_in[j].astype(F32)
        result_ref[:, piece_columns(j)] = (whole * scale_row).astype(BF16)
        return 0

    lax.fori_loop(0, pieces, collect, 0)

    link_copy(1).wait_send()
    left(fresh_own.at[:, 0], fresh_send.at[1])

    @pl.when(core == 0)
    def _():
        link_copy(0).wait_send()
        left(fresh_own.at[:, 0], fresh_send.at[0])

    @pl.when(carries & (pair < last_pair))
    def _():
        left(chain_out, chain_send)

    @pl.when(carries & (cross > 0))
    def _():
        left(states.at[0], return_send.at[1])

    @pl.when(carries & (s > 0))
    def _():
        left(states.at[0, :, 0], return_send.at[0])

    left(square_out.at[pl.ds(0, 3)], square_send)

    @pl.when(core == 0)
    def _():
        left(near_out, near_send)
        left(far_out.at[pl.ds(0, pieces - 1)], far_send)

    @pl.when(carries)
    def _():
        left(near_out.at[pl.ds(0, 2 * pieces - 1)], near_send)
        left(far_out, far_send)

    left(extra_out, extra_send)

    def drain_relay(i, _):
        @pl.when(i < borrowed)
        def _():
            relay_copy(i).wait_send()

        return 0

    lax.fori_loop(0, SLOTS, drain_relay, 0)


def local(
    n_seq,
    n_head,
    stream,
    gate_input,
    in_coeff,
    out_coeff,
    step_raw,
    step_bias,
    decay_rate,
    skip_scale,
    norm_gain,
    out_proj,
    doc_starts,
):
    rows, channels = stream.shape
    heads = step_raw.shape[0]
    state = in_coeff.shape[1]
    model = out_proj.shape[1]
    chunks, pieces = channels // 256, model // 256
    width, piece = channels // chunks, model // pieces
    sub = width // 2
    padded = -(-heads // 8) * 8
    share = rows // n_head
    assert n_head == 4 and n_seq % 2 == 0 and rows <= 512
    vmem = pl.BlockSpec(memory_space=pltpu.VMEM)
    anywhere = pl.BlockSpec(memory_space=pl.ANY)
    dma = pltpu.SemaphoreType.DMA
    return pl.pallas_call(
        functools.partial(kernel, n_seq, n_head, heads, chunks, pieces),
        out_shape=pltpu.VMEM((share, model), BF16),
        in_specs=[anywhere] * 11,
        out_specs=vmem,
        scratch_shapes=[
            pltpu.VMEM(doc_starts.shape, doc_starts.dtype),
            pltpu.VMEM(step_raw.shape, F32),
            pltpu.VMEM((1, heads), F32),
            pltpu.VMEM((1, heads), F32),
            pltpu.VMEM((1, heads), F32),
            pltpu.VMEM(norm_gain.shape, F32),
            pltpu.VMEM(in_coeff.shape, BF16),
            pltpu.VMEM(out_coeff.shape, BF16),
            pltpu.VMEM((rows, channels), BF16),
            pltpu.VMEM((rows, channels), BF16),
            pltpu.VMEM((channels, model), BF16),
            pltpu.VMEM((padded, rows), F32),
            pltpu.VMEM((2 * padded, channels), BF16),
            pltpu.VMEM((2 * padded, rows), BF16),
            pltpu.VMEM((2 * padded, rows), BF16),
            pltpu.VMEM((rows, rows), BF16),
            pltpu.VMEM((rows, state), BF16),
            pltpu.VMEM((rows, channels), BF16),
            pltpu.VMEM((1, channels), F32),
            pltpu.VMEM((4, 1, channels), F32),
            pltpu.VMEM((8, channels), F32),
            pltpu.VMEM((rows, channels), F32),
            pltpu.VMEM((rows, channels), F32),
            pltpu.VMEM((rows, 128), F32),
            pltpu.VMEM((rows, channels), BF16),
            pltpu.VMEM((chunks, 2, state, sub), BF16),
            pltpu.VMEM((chunks, 4, state, sub), BF16),
            pltpu.VMEM((chunks, 2, state, sub), BF16),
            pltpu.VMEM((2, chunks, 2, state, sub), BF16),
            pltpu.VMEM((chunks, 2, state, sub), BF16),
            pltpu.VMEM((n_head, 8, share), F32),
            pltpu.VMEM((n_head - 1, 8, share), F32),
            pltpu.VMEM((2 * pieces, 2 * share, piece), F32),
            pltpu.VMEM((2 * pieces, share, piece), BF16),
            pltpu.VMEM((2 * pieces, share, piece), BF16),
            pltpu.VMEM((pieces, share, piece), BF16),
            pltpu.VMEM((pieces, share, piece), BF16),
            pltpu.VMEM((SLOTS, share, piece), BF16),
            pltpu.VMEM((share, piece), BF16),
            pltpu.VMEM((share, piece), BF16),
            dma((8,)),
            dma((3,)),
            pltpu.SemaphoreType.REGULAR,
            dma((2,)),
            dma,
            dma((2,)),
            dma((chunks,)),
            dma,
            dma((chunks, 2)),
            dma((2,)),
            dma((chunks,)),
            dma,
            dma,
            dma,
            dma((pieces,)),
            dma,
            dma,
            dma((pieces,)),
            dma((SLOTS,)),
            dma((SLOTS,)),
            dma,
            dma,
        ],
        compiler_params=pltpu.CompilerParams(
            collective_id=0, has_side_effects=True, vmem_limit_bytes=56 * 1024 * 1024
        ),
    )(
        doc_starts,
        step_raw,
        step_bias.reshape(1, -1),
        decay_rate.reshape(1, -1),
        skip_scale.reshape(1, -1),
        norm_gain,
        in_coeff,
        out_coeff,
        stream,
        gate_input,
        out_proj,
    )


def solution(mesh):
    in_specs = (
        P("seq", "head"),
        P("seq", "head"),
        P("seq", None),
        P("seq", None),
        P("head", "seq"),
        P("head"),
        P("head"),
        P("head"),
        P("head"),
        P("head", None),
        P(),
    )
    out_specs = P(("seq", "head"), None)
    body = functools.partial(local, mesh.shape["seq"], mesh.shape["head"])
    return jax.shard_map(body, mesh=mesh, in_specs=in_specs, out_specs=out_specs, check_vma=False)
```

```python
import functools

import jax
import jax.numpy as jnp
from jax import lax
from jax.experimental import pallas as pl
from jax.experimental.pallas import tpu as pltpu
from jax.sharding import PartitionSpec as P

EPSILON = 1e-05
F32 = jnp.float32
BF16 = jnp.bfloat16
MESH = pl.DeviceIdType.MESH
LEAD = 1
LEND_FROM = 2
FAR_LAG = 2
READY = 2
SOON = 1
LAG = 3
LENT = ((2, 2), (1, 0))
SLOTS = max(max(counts) for counts in LENT)


def dot(a, b, ca, cb):
    return lax.dot_general(a, b, (((ca,), (cb,)), ((), ())), preferred_element_type=F32)


def split(value, parts):
    pieces = []
    for _ in range(parts):
        piece = value.astype(BF16).astype(F32)
        pieces.append(piece)
        value = value - piece
    return jnp.concatenate(pieces, axis=0).astype(BF16)


def to_column(row):
    n = row.shape[1]
    eye = lax.broadcasted_iota(jnp.int32, (n, n), 0) == lax.broadcasted_iota(jnp.int32, (n, n), 1)
    return jnp.sum(jnp.where(eye, row, 0.0), axis=1, keepdims=True)


def lends(pair, last_pair, core):
    if last_pair + 1 < 2 * len(LENT):
        return 0 * pair
    return sum(
        jnp.where(pair == last_pair - i, jnp.where(core == 0, *counts), 0)
        for i, counts in enumerate(LENT)
    )


def kernel(
    n_seq,
    n_head,
    heads,
    chunks,
    pieces,
    starts_hbm,
    step_hbm,
    bias_hbm,
    rate_hbm,
    skip_hbm,
    gain_hbm,
    in_hbm,
    out_hbm,
    stream_hbm,
    gate_hbm,
    proj_hbm,
    result_ref,
    starts_ref,
    step_ref,
    bias_ref,
    rate_ref,
    skip_ref,
    gain_ref,
    in_ref,
    out_ref,
    stream,
    gate,
    proj,
    pad,
    expand,
    factor_in,
    factor_out,
    pairs,
    carry_in,
    source,
    link_own,
    link_all,
    before_gate,
    base,
    slope,
    square,
    hidden,
    fresh_own,
    fresh_all,
    chain_out,
    states,
    incoming_all,
    square_out,
    square_in,
    held,
    outbox,
    near_in,
    far_in,
    relay_in,
    extra_in,
    small_sem,
    load_sem,
    ready_sem,
    link_send,
    link_recv,
    fresh_send,
    fresh_recv,
    chain_send,
    chain_recv,
    return_send,
    return_recv,
    square_send,
    square_recv,
    sent,
    near_recv,
    near_last,
    far_recv,
    relay_send,
    relay_recv,
    extra_recv,
):
    rows, channels = stream.shape
    state = in_ref.shape[1]
    width = channels // chunks
    head_size = channels // heads
    padded = pad.shape[0]
    sub = width // 2
    half = rows // 2
    share = rows // n_head
    piece = proj.shape[1] // pieces

    s = lax.axis_index("seq")
    g = lax.axis_index("head")
    parity = s % 2
    pair = s // 2
    last_pair = n_seq // 2 - 1
    core = g % 2
    side = g // 2
    near = side * 2 + (1 - core)
    far = (1 - side) * 2 + core
    cross = s + 1 - 2 * parity
    carrier = 2 * side + 1
    carries = core == 1
    helped = last_pair - pair
    lent = lends(pair, last_pair, core)
    borrowed = lends(helped, last_pair, core)
    helper = 2 * helped + parity
    peers = (near, far, (1 - side) * 2 + (1 - core))

    loads = [
        pltpu.make_async_copy(src, dst, load_sem.at[i])
        for i, (src, dst) in enumerate(((stream_hbm, stream), (gate_hbm, gate), (proj_hbm, proj)))
    ]
    smalls = [
        pltpu.make_async_copy(src, dst, small_sem.at[i])
        for i, (src, dst) in enumerate(
            (
                (step_hbm, step_ref),
                (bias_hbm, bias_ref),
                (rate_hbm, rate_ref),
                (starts_hbm, starts_ref),
                (in_hbm, in_ref),
                (skip_hbm, skip_ref),
                (gain_hbm, gain_ref),
                (out_hbm, out_ref),
            )
        )
    ]
    for small in smalls[:5]:
        small.start()
    loads[0].start()
    for small in smalls[5:]:
        small.start()

    barrier = pltpu.get_barrier_semaphore()
    for peer in peers:
        pl.semaphore_signal(barrier, inc=1, device_id=(s, peer), device_id_type=MESH)
    for peer in (g, near):
        pl.semaphore_signal(barrier, inc=1, device_id=(cross, peer), device_id_type=MESH)

    @pl.when(pair < last_pair)
    def _():
        pl.semaphore_signal(barrier, inc=1, device_id=(s + 2, g), device_id_type=MESH)

    @pl.when(borrowed > 0)
    def _():
        pl.semaphore_signal(barrier, inc=1, device_id=(helper, far), device_id_type=MESH)

    def remote(src, dst, send_sem, recv_sem, seq, head):
        return pltpu.make_async_remote_copy(
            src_ref=src,
            dst_ref=dst,
            send_sem=send_sem,
            recv_sem=recv_sem,
            device_id=(seq, head),
            device_id_type=MESH,
        )

    def slot(part, away):
        return 2 * part + 1 - away

    def link_copy(away):
        return remote(
            link_own,
            link_all.at[slot(core, away)],
            link_send.at[away],
            link_recv,
            cross if away else s,
            carrier,
        )

    def fresh_copy(k, away):
        return remote(
            fresh_own.at[k, 1 - parity if away else parity],
            fresh_all.at[k, slot(core, away)],
            fresh_send,
            fresh_recv.at[k],
            cross if away else s,
            carrier,
        )

    def chain_copy(k, part):
        return remote(
            chain_out.at[k, part],
            states.at[0, k, part],
            chain_send,
            chain_recv.at[k, part],
            (s + 2) % n_seq,
            g,
        )

    def return_copy(k, away, part, owner):
        return remote(
            states.at[1 - parity if away else parity, k, part],
            incoming_all.at[k, owner],
            return_send.at[away],
            return_recv.at[k],
            cross if away else s,
            2 * side + part,
        )

    def arrived(dst, sem):
        remote(dst, dst, sem, sem, s, near).wait_recv()

    def left(src, sem):
        remote(src, src, sem, sem, s, near).wait_send()

    pad[...] = jnp.zeros_like(pad)
    head_row = lax.broadcasted_iota(jnp.int32, (padded, channels), 0) * head_size
    lane = lax.broadcasted_iota(jnp.int32, (padded, channels), 1)
    spread = jnp.where((lane >= head_row) & (lane < head_row + head_size), 1.0, 0.0)
    expand[...] = jnp.concatenate([spread, spread], axis=0).astype(BF16)
    first = lax.broadcasted_iota(jnp.int32, (rows, rows), 0)
    second = lax.broadcasted_iota(jnp.int32, (rows, rows), 1)
    upper = jnp.where(first <= second, 1.0, 0.0).astype(BF16)
    pairs[...] = upper
    for small in smalls[:5]:
        small.wait()
    raw = step_ref[...] + to_column(bias_ref[...])
    pad[pl.ds(0, heads), :] = jnp.maximum(raw, 0.0) + jnp.log(1.0 + jnp.exp(-jnp.abs(raw)))
    step_size = pad[...]
    rate = to_column(rate_ref[...])
    if padded > heads:
        rate = jnp.concatenate([rate, jnp.zeros((padded - heads, 1), F32)], axis=0)
    log_decay = -step_size * rate
    sums = dot(split(log_decay, 3), pairs[...], 1, 0)
    cumulative = sums[:padded] + sums[padded : 2 * padded] + sums[2 * padded :]
    middle = cumulative[:, half - 1 : half]
    last = cumulative[:, rows - 1 : rows]
    factor_in[...] = split(jnp.exp(middle - cumulative) * step_size, 2)

    starts = starts_ref[...].astype(F32).reshape(1, -1)
    offset = s * rows
    place = (offset + lax.broadcasted_iota(jnp.int32, (rows, 1), 0)).astype(F32)
    place_lane = (offset + lax.broadcasted_iota(jnp.int32, (1, rows), 1)).astype(F32)
    doc = jnp.sum(jnp.where(starts <= place, 1.0, 0.0), axis=1, keepdims=True)
    before = jnp.sum(jnp.where(starts <= (offset - 1).astype(F32), 1.0, 0.0), axis=1, keepdims=True)
    doc_end = doc[rows - 1 : rows, :]
    joined_end = jnp.where(doc_end == before, 1.0, 0.0)

    def per_channel(column):
        return jnp.sum(spread * column, axis=0, keepdims=True)

    link_own[...] = per_channel(jnp.exp(last)) * joined_end
    end_gate = per_channel(jnp.exp(last - middle))
    before_gate[1:2, :] = end_gate
    in_end = jnp.where(doc == doc_end, in_ref[...].astype(F32), 0.0).astype(BF16)

    loads[0].wait()
    loads[1].start()
    loads[2].start()

    def columns(k):
        return pl.ds(pl.multiple_of(k * width, width), width)

    def meet():
        greetings = len(peers) + 2 + (pair > 0).astype(jnp.int32) + (lent > 0).astype(jnp.int32)
        pl.semaphore_wait(barrier, greetings)

        @pl.when(carries & (pair > 0))
        def _():
            pl.semaphore_signal(ready_sem, inc=1, device_id=(s - 2, g), device_id_type=MESH)

        link_copy(1).start()

        @pl.when(core == 0)
        def _():
            link_copy(0).start()

        @pl.when(carries)
        def _():
            link_all[3] = link_own[...]

    def make_summary(k, _):
        cols = columns(k)
        scale = dot(factor_in[...], expand[:, cols], 0, 0)
        scaled = (stream[:, cols].astype(F32) * scale).astype(BF16)
        source[:, cols] = scaled
        fresh = dot(in_end, scaled, 0, 0) * before_gate[1:2, cols]

        for i in range(2):
            fresh_own[k, i] = fresh[:, i * sub : (i + 1) * sub].astype(BF16)
        @pl.when((k == 0) & carries)
        def _():
            meet()

        fresh_copy(k, 1).start()

        @pl.when(core == 0)
        def _():
            fresh_copy(k, 0).start()

        @pl.when(carries)
        def _():
            fresh_all[k, 3] = fresh_own[k, parity]

        return 0

    @pl.when(core == 0)
    def _():
        meet()

    lax.fori_loop(0, chunks, make_summary, 0)

    for small in smalls[5:]:
        small.wait()

    factor_out[...] = split(jnp.exp(cumulative - middle), 2)
    before_gate[3:4, :] = gain_ref[...].reshape(1, -1)
    doc_lane = jnp.sum(jnp.where(to_column(starts) <= place_lane, 1.0, 0.0), axis=0, keepdims=True)
    before_gate[0:1, :] = per_channel(jnp.exp(middle))
    skip = to_column(skip_ref[...])
    if padded > heads:
        skip = jnp.concatenate([skip, jnp.zeros((padded - heads, 1), F32)], axis=0)
    before_gate[2:3, :] = per_channel(skip)
    carry_in[...] = jnp.where(doc == before, out_ref[...].astype(F32), 0.0).astype(BF16)
    scores = dot(out_ref[...], in_ref[...], 1, 1)
    live = (first >= second) & (doc == doc_lane)
    pairs[...] = jnp.where(live, scores, 0.0).astype(BF16)
    square[...] = jnp.zeros_like(square)
    loads[1].wait()

    @pl.when(s == 0)
    def _():
        incoming_all[...] = jnp.zeros_like(incoming_all)

    def local_part(k):
        cols = columns(k)
        gate_value = gate[:, cols].astype(F32)
        silu = gate_value * (0.5 * jnp.tanh(0.5 * gate_value) + 0.5)
        within = jnp.concatenate(
            [
                dot(pairs[:half, :half], source[:half, cols], 1, 0),
                dot(pairs[half:, :], source[:, cols], 1, 0),
            ],
            axis=0,
        )
        factor = dot(factor_out[...], expand[:, cols], 0, 0) * silu
        slope[:, cols] = factor
        base[:, cols] = within * factor + stream[:, cols].astype(F32) * before_gate[2:3, cols] * silu

    def chain_step(k):
        cols = pl.ds(pl.multiple_of(k * width + parity * sub, sub), sub)

        @pl.when(k == 0)
        def _():
            arrived(link_all.at[pl.ds(0, 3)], link_recv)

        arrived(fresh_all.at[k, pl.ds(0, 3)], fresh_recv.at[k])

        for part in range(2):
            even, odd = 2 * part + 1 - parity, 2 * part + parity
            keep_even, keep_odd = link_all[even, :, cols], link_all[odd, :, cols]
            fresh_even = fresh_all[k, even].astype(F32)
            fresh_odd = fresh_all[k, odd].astype(F32)

            @pl.when(pair > 0)
            def _():
                chain_copy(k, part).wait_recv()
                between = keep_even * states[0, k, part].astype(F32) + fresh_even
                states[1, k, part] = between.astype(BF16)
                chain_out[k, part] = (keep_odd * between + fresh_odd).astype(BF16)

            @pl.when(pair == 0)
            def _():
                states[1, k, part] = fresh_all[k, even]
                chain_out[k, part] = (keep_odd * fresh_even + fresh_odd).astype(BF16)

            @pl.when(pair < last_pair)
            def _():
                chain_copy(k, part).start()

            @pl.when(cross > 0)
            def _():
                return_copy(k, 1, part, parity).start()

            @pl.when(s > 0)
            def _():
                if part == 0:
                    return_copy(k, 0, part, parity).start()
                else:
                    incoming_all[k, parity] = states[parity, k, part]

    def take(k):
        @pl.when(carries & (s > 0))
        def _():
            arrived(incoming_all.at[k, 0], return_recv.at[k])

        @pl.when((core == 0) & (s > 0))
        def _():
            arrived(incoming_all.at[k], return_recv.at[k])

    def half_rows(which):
        return pl.ds(pl.multiple_of(which * half, half), half)

    def piece_columns(j):
        return pl.ds(pl.multiple_of(j * piece, piece), piece)

    def finish(k, span):
        cols = columns(k)
        incoming = jnp.concatenate([incoming_all[k, i].astype(F32) for i in range(2)], axis=1)
        incoming = (incoming * before_gate[0:1, cols]).astype(BF16)
        carried = dot(carry_in[span, :], incoming, 1, 0)
        gated = base[span, cols] + slope[span, cols] * carried
        hidden[span, cols] = (gated * before_gate[3:4, cols]).astype(BF16)
        squares = gated * gated
        total = square[span, :]
        for i in range(width // 128):
            total = total + squares[:, i * 128 : (i + 1) * 128]
        square[span, :] = total

    def product(span, depth, j):
        return dot(hidden[span, depth], proj[depth, piece_columns(j)], 1, 0)

    early_depth = pl.ds(0, channels - width)
    late_depth = pl.ds(channels - width, width)

    lead = jnp.where(pair == 0, LEAD, chunks)


    def main_step(step, _):
        @pl.when(carries & (step >= lead) & (step < lead + chunks))
        def _():
            chain_step(step - lead)

        @pl.when(step < chunks)
        def _():
            local_part(step)

        @pl.when(carries & (step >= lead + LAG))
        def _():
            take(step - lead - LAG)
            finish(step - lead - LAG, pl.ds(0, rows))

        return 0

    @pl.when(carries & (pair < last_pair))
    def _():
        pl.semaphore_wait(ready_sem, 1)

    lax.fori_loop(0, chunks + jnp.where(carries, lead, 0), main_step, 0)

    loads[2].wait()

    def finish_step(k, _):
        take(k)
        finish(k, pl.ds(0, rows))
        return 0

    lax.fori_loop(jnp.where(carries, chunks - LAG, 0), chunks - 1, finish_step, 0)
    for j in range(READY):
        held[j] = product(half_rows(1 - side), early_depth, j)
    take(chunks - 1)
    finish(chunks - 1, half_rows(1 - side))

    def near_copy(stage, j, sem):
        at = stage * pieces + j
        return remote(outbox.at[at], near_in.at[at], sent, sem, s, near)

    def place(j):
        return jnp.maximum(j - (pieces - 5), 0)

    def far_copy(j):
        return remote(outbox.at[2 * pieces + j], far_in.at[j], sent, far_recv.at[place(j)], s, far)

    def lend_copy(j):
        return remote(
            outbox.at[2 * pieces + j],
            relay_in.at[j - LEND_FROM],
            sent,
            relay_recv.at[j - LEND_FROM],
            helper,
            far,
        )

    def relay_copy(i):
        return remote(
            relay_in.at[i],
            far_in.at[i + LEND_FROM],
            relay_send,
            far_recv.at[place(i + LEND_FROM)],
            helper,
            g,
        )

    def core_rows(which):
        return pl.ds(pl.multiple_of(which * share, share), share)

    def extra_copy():
        return remote(outbox.at[3 * pieces], extra_in, sent, extra_recv, s, near)

    def extra_far_copy():
        return remote(
            outbox.at[3 * pieces], far_in.at[pieces - 1], sent, far_recv.at[4], s, 2 * (1 - side)
        )

    def exchange(stage, j):
        at = stage * pieces + j
        outbox[at] = held[at, core_rows(1 - core), :].astype(BF16)
        near_copy(stage, j, near_recv.at[j] if stage == 0 else near_last).start()

    def project(stage, which, j):
        at = stage * pieces + j
        held[at] = product(half_rows(which), pl.ds(0, channels), j)

    def pass_on(j):
        near_copy(0, j, near_recv.at[j]).wait_recv()
        both = held[j, core_rows(core), :] + near_in[j].astype(F32)
        outbox[2 * pieces + j] = both.astype(BF16)
        lend = (j >= LEND_FROM) & (j < LEND_FROM + lent)

        @pl.when(lend)
        def _():
            lend_copy(j).start()

        @pl.when(jnp.logical_not(lend))
        def _():
            far_copy(j).start()

    def pass_on_extra():
        extra_copy().wait_recv()
        both = held[pieces - 1, core_rows(1 - core), :] + extra_in[...].astype(F32)
        outbox[3 * pieces] = both.astype(BF16)
        extra_far_copy().start()

    def square_copy(i):
        return remote(
            square_out.at[peers[i]], square_in.at[i], square_send, square_recv, s, peers[i]
        )

    def send_squares():
        for owner in range(n_head):
            block = square[owner * share : (owner + 1) * share, :]
            sums_lane = jnp.sum(block.T, axis=0, keepdims=True)
            square_out[owner] = sums_lane
        for i in range(len(peers)):
            square_copy(i).start()

    def far_step(j, _):
        @pl.when(j < READY)
        def _():
            held[j] = held[j] + product(half_rows(1 - side), late_depth, j)

        @pl.when((j >= READY) & (j < pieces))
        def _():
            project(0, 1 - side, j)

        @pl.when((j < pieces - 1) | ((j == pieces - 1) & (core == 0)))
        def _():
            exchange(0, j)

        @pl.when((j == pieces - 1) & (core == 0))
        def _():
            outbox[3 * pieces] = held[pieces - 1, core_rows(core), :].astype(BF16)
            extra_copy().start()

        @pl.when(j == SOON)
        def _():
            pass_on(0)
            finish(chunks - 1, half_rows(side))
            send_squares()

        @pl.when(carries & (j == pieces + FAR_LAG - 1))
        def _():
            pass_on_extra()

        @pl.when((j > FAR_LAG) & (carries | (j < pieces + FAR_LAG - 1)))
        def _():
            pass_on(j - FAR_LAG)

        return 0

    lax.fori_loop(0, pieces + FAR_LAG, far_step, 0)

    def near_step(j, _):
        project(1, side, j)
        exchange(1, j)
        return 0

    lax.fori_loop(0, pieces, near_step, 0)

    def relay_step(i, _):
        @pl.when(i < borrowed)
        def _():
            arrived(relay_in.at[i], relay_recv.at[i])
            relay_copy(i).start()

        return 0

    lax.fori_loop(0, SLOTS, relay_step, 0)

    arrived(square_in, square_recv)
    total = square_out[g]
    for i in range(len(peers)):
        total = total + square_in[i]
    mean = jnp.broadcast_to(total, (128, share)).T / (channels * n_head)
    scale_row = lax.rsqrt(mean + EPSILON)[:, 0:1]

    arrived(near_in.at[pl.ds(pieces, pieces)], near_last)

    arrived(far_in.at[pl.ds(0, pieces - 4)], far_recv.at[0])

    def collect(j, _):
        @pl.when(j > pieces - 5)
        def _():
            far_copy(j).wait_recv()

        at = pieces + j
        whole = held[at, core_rows(core), :] + near_in[at].astype(F32) + far_in[j].astype(F32)
        result_ref[:, piece_columns(j)] = (whole * scale_row).astype(BF16)
        return 0

    lax.fori_loop(0, pieces, collect, 0)

    link_copy(1).wait_send()

    @pl.when(core == 0)
    def _():
        link_copy(0).wait_send()
        left(fresh_own, fresh_send)

    @pl.when(carries)
    def _():
        left(fresh_own.at[:, 0], fresh_send)

    @pl.when(carries & (pair < last_pair))
    def _():
        left(chain_out, chain_send)

    @pl.when(carries & (cross > 0))
    def _():
        left(states.at[0], return_send.at[1])

    @pl.when(carries & (s > 0))
    def _():
        left(states.at[0, :, 0], return_send.at[0])

    left(square_out.at[pl.ds(0, 3)], square_send)
    left(outbox.at[pl.ds(0, 3 * pieces)], sent)

    for count in range(1, SLOTS + 1):

        @pl.when(borrowed == count)
        def _():
            left(relay_in.at[pl.ds(0, count)], relay_send)


def local(
    n_seq,
    n_head,
    stream,
    gate_input,
    in_coeff,
    out_coeff,
    step_raw,
    step_bias,
    decay_rate,
    skip_scale,
    norm_gain,
    out_proj,
    doc_starts,
):
    rows, channels = stream.shape
    heads = step_raw.shape[0]
    state = in_coeff.shape[1]
    model = out_proj.shape[1]
    chunks, pieces = channels // 256, model // 256
    width, piece = channels // chunks, model // pieces
    sub = width // 2
    padded = -(-heads // 8) * 8
    share = rows // n_head
    assert n_head == 4 and n_seq % 2 == 0 and rows <= 512
    vmem = pl.BlockSpec(memory_space=pltpu.VMEM)
    anywhere = pl.BlockSpec(memory_space=pl.ANY)
    dma = pltpu.SemaphoreType.DMA
    return pl.pallas_call(
        functools.partial(kernel, n_seq, n_head, heads, chunks, pieces),
        out_shape=pltpu.VMEM((share, model), BF16),
        in_specs=[anywhere] * 11,
        out_specs=vmem,
        scratch_shapes=[
            pltpu.VMEM(doc_starts.shape, doc_starts.dtype),
            pltpu.VMEM(step_raw.shape, F32),
            pltpu.VMEM((1, heads), F32),
            pltpu.VMEM((1, heads), F32),
            pltpu.VMEM((1, heads), F32),
            pltpu.VMEM(norm_gain.shape, F32),
            pltpu.VMEM(in_coeff.shape, BF16),
            pltpu.VMEM(out_coeff.shape, BF16),
            pltpu.VMEM((rows, channels), BF16),
            pltpu.VMEM((rows, channels), BF16),
            pltpu.VMEM((channels, model), BF16),
            pltpu.VMEM((padded, rows), F32),
            pltpu.VMEM((2 * padded, channels), BF16),
            pltpu.VMEM((2 * padded, rows), BF16),
            pltpu.VMEM((2 * padded, rows), BF16),
            pltpu.VMEM((rows, rows), BF16),
            pltpu.VMEM((rows, state), BF16),
            pltpu.VMEM((rows, channels), BF16),
            pltpu.VMEM((1, channels), F32),
            pltpu.VMEM((4, 1, channels), F32),
            pltpu.VMEM((8, channels), F32),
            pltpu.VMEM((rows, channels), F32),
            pltpu.VMEM((rows, channels), F32),
            pltpu.VMEM((rows, 128), F32),
            pltpu.VMEM((rows, channels), BF16),
            pltpu.VMEM((chunks, 2, state, sub), BF16),
            pltpu.VMEM((chunks, 4, state, sub), BF16),
            pltpu.VMEM((chunks, 2, state, sub), BF16),
            pltpu.VMEM((2, chunks, 2, state, sub), BF16),
            pltpu.VMEM((chunks, 2, state, sub), BF16),
            pltpu.VMEM((n_head, 1, share), F32),
            pltpu.VMEM((n_head - 1, 1, share), F32),
            pltpu.VMEM((2 * pieces, 2 * share, piece), F32),
            pltpu.VMEM((3 * pieces + 1, share, piece), BF16),
            pltpu.VMEM((2 * pieces, share, piece), BF16),
            pltpu.VMEM((pieces, share, piece), BF16),
            pltpu.VMEM((SLOTS, share, piece), BF16),
            pltpu.VMEM((share, piece), BF16),
            dma((8,)),
            dma((3,)),
            pltpu.SemaphoreType.REGULAR,
            dma((2,)),
            dma,
            dma,
            dma((chunks,)),
            dma,
            dma((chunks, 2)),
            dma((2,)),
            dma((chunks,)),
            dma,
            dma,
            dma,
            dma((pieces,)),
            dma,
            dma((5,)),
            dma,
            dma((SLOTS,)),
            dma,
        ],
        compiler_params=pltpu.CompilerParams(
            collective_id=0, has_side_effects=True, vmem_limit_bytes=56 * 1024 * 1024
        ),
    )(
        doc_starts,
        step_raw,
        step_bias.reshape(1, -1),
        decay_rate.reshape(1, -1),
        skip_scale.reshape(1, -1),
        norm_gain,
        in_coeff,
        out_coeff,
        stream,
        gate_input,
        out_proj,
    )


def solution(mesh):
    in_specs = (
        P("seq", "head"),
        P("seq", "head"),
        P("seq", None),
        P("seq", None),
        P("head", "seq"),
        P("head"),
        P("head"),
        P("head"),
        P("head"),
        P("head", None),
        P(),
    )
    out_specs = P(("seq", "head"), None)
    body = functools.partial(local, mesh.shape["seq"], mesh.shape["head"])
    return jax.shard_map(body, mesh=mesh, in_specs=in_specs, out_specs=out_specs, check_vma=False)
```

```python
import functools

import jax
import jax.numpy as jnp
from jax import lax
from jax.experimental import pallas as pl
from jax.experimental.pallas import tpu as pltpu
from jax.sharding import PartitionSpec as P

EPSILON = 1e-05
F32 = jnp.float32
BF16 = jnp.bfloat16
MESH = pl.DeviceIdType.MESH
LEAD = 1
LEND_FROM = 2
FAR_LAG = 2
READY = 2
SOON = 1
LAG = 3
LENT = ((2, 2), (1, 0))
SLOTS = max(max(counts) for counts in LENT)


def dot(a, b, ca, cb):
    return lax.dot_general(a, b, (((ca,), (cb,)), ((), ())), preferred_element_type=F32)


def split(value, parts):
    pieces = []
    for _ in range(parts):
        piece = value.astype(BF16).astype(F32)
        pieces.append(piece)
        value = value - piece
    return jnp.concatenate(pieces, axis=0).astype(BF16)


def to_column(row):
    n = row.shape[1]
    eye = lax.broadcasted_iota(jnp.int32, (n, n), 0) == lax.broadcasted_iota(jnp.int32, (n, n), 1)
    return jnp.sum(jnp.where(eye, row, 0.0), axis=1, keepdims=True)


def lends(pair, last_pair, core):
    if last_pair + 1 < 2 * len(LENT):
        return 0 * pair
    return sum(
        jnp.where(pair == last_pair - i, jnp.where(core == 0, *counts), 0)
        for i, counts in enumerate(LENT)
    )


def kernel(
    n_seq,
    n_head,
    heads,
    chunks,
    pieces,
    starts_hbm,
    step_hbm,
    bias_hbm,
    rate_hbm,
    skip_hbm,
    gain_hbm,
    in_hbm,
    out_hbm,
    stream_hbm,
    gate_hbm,
    proj_hbm,
    result_ref,
    starts_ref,
    step_ref,
    bias_ref,
    rate_ref,
    skip_ref,
    gain_ref,
    in_ref,
    out_ref,
    stream,
    gate,
    proj,
    pad,
    expand,
    factor_in,
    factor_out,
    pairs,
    carry_in,
    source,
    link_own,
    link_all,
    before_gate,
    base,
    slope,
    square,
    hidden,
    fresh_own,
    fresh_all,
    chain_out,
    states,
    incoming_all,
    square_out,
    square_in,
    held,
    outbox,
    near_in,
    far_in,
    relay_in,
    extra_in,
    small_sem,
    load_sem,
    ready_sem,
    link_send,
    link_recv,
    fresh_send,
    fresh_recv,
    chain_send,
    chain_recv,
    return_send,
    return_recv,
    square_send,
    square_recv,
    sent,
    near_recv,
    near_last,
    far_recv,
    relay_send,
    relay_recv,
    extra_recv,
):
    rows, channels = stream.shape
    state = in_ref.shape[1]
    width = channels // chunks
    head_size = channels // heads
    padded = pad.shape[0]
    sub = width // 2
    half = rows // 2
    share = rows // n_head
    piece = proj.shape[1] // pieces

    s = lax.axis_index("seq")
    g = lax.axis_index("head")
    parity = s % 2
    pair = s // 2
    last_pair = n_seq // 2 - 1
    core = g % 2
    side = g // 2
    near = side * 2 + (1 - core)
    far = (1 - side) * 2 + core
    cross = s + 1 - 2 * parity
    carrier = 2 * side + 1
    carries = core == 1
    helped = last_pair - pair
    lent = lends(pair, last_pair, core)
    borrowed = lends(helped, last_pair, core)
    helper = 2 * helped + parity
    peers = (near, far, (1 - side) * 2 + (1 - core))

    loads = [
        pltpu.make_async_copy(src, dst, load_sem.at[i])
        for i, (src, dst) in enumerate(((stream_hbm, stream), (gate_hbm, gate), (proj_hbm, proj)))
    ]
    smalls = [
        pltpu.make_async_copy(src, dst, small_sem.at[i])
        for i, (src, dst) in enumerate(
            (
                (step_hbm, step_ref),
                (bias_hbm, bias_ref),
                (rate_hbm, rate_ref),
                (starts_hbm, starts_ref),
                (in_hbm, in_ref),
                (skip_hbm, skip_ref),
                (gain_hbm, gain_ref),
                (out_hbm, out_ref),
            )
        )
    ]
    for small in smalls[:5]:
        small.start()
    loads[0].start()
    for small in smalls[5:]:
        small.start()

    barrier = pltpu.get_barrier_semaphore()
    for peer in peers:
        pl.semaphore_signal(barrier, inc=1, device_id=(s, peer), device_id_type=MESH)
    for peer in (g, near):
        pl.semaphore_signal(barrier, inc=1, device_id=(cross, peer), device_id_type=MESH)

    @pl.when(pair < last_pair)
    def _():
        pl.semaphore_signal(barrier, inc=1, device_id=(s + 2, g), device_id_type=MESH)

    @pl.when(borrowed > 0)
    def _():
        pl.semaphore_signal(barrier, inc=1, device_id=(helper, far), device_id_type=MESH)

    def remote(src, dst, send_sem, recv_sem, seq, head):
        return pltpu.make_async_remote_copy(
            src_ref=src,
            dst_ref=dst,
            send_sem=send_sem,
            recv_sem=recv_sem,
            device_id=(seq, head),
            device_id_type=MESH,
        )

    def slot(part, away):
        return 2 * part + 1 - away

    def link_copy(away):
        return remote(
            link_own,
            link_all.at[slot(core, away)],
            link_send.at[away],
            link_recv,
            cross if away else s,
            carrier,
        )

    def fresh_copy(k, away):
        return remote(
            fresh_own.at[k, 1 - parity if away else parity],
            fresh_all.at[k, slot(core, away)],
            fresh_send,
            fresh_recv.at[k],
            cross if away else s,
            carrier,
        )

    def chain_copy(k, part):
        return remote(
            chain_out.at[k, part],
            states.at[0, k, part],
            chain_send,
            chain_recv.at[k, part],
            (s + 2) % n_seq,
            g,
        )

    def return_copy(k, away, part, owner):
        return remote(
            states.at[1 - parity if away else parity, k, part],
            incoming_all.at[k, owner],
            return_send.at[away],
            return_recv.at[k],
            cross if away else s,
            2 * side + part,
        )

    def arrived(dst, sem):
        remote(dst, dst, sem, sem, s, near).wait_recv()

    def left(src, sem):
        remote(src, src, sem, sem, s, near).wait_send()

    pad[...] = jnp.zeros_like(pad)
    head_row = lax.broadcasted_iota(jnp.int32, (padded, channels), 0) * head_size
    lane = lax.broadcasted_iota(jnp.int32, (padded, channels), 1)
    spread = jnp.where((lane >= head_row) & (lane < head_row + head_size), 1.0, 0.0)
    expand[...] = jnp.concatenate([spread, spread], axis=0).astype(BF16)
    first = lax.broadcasted_iota(jnp.int32, (rows, rows), 0)
    second = lax.broadcasted_iota(jnp.int32, (rows, rows), 1)
    upper = jnp.where(first <= second, 1.0, 0.0).astype(BF16)
    pairs[...] = upper
    for small in smalls[:5]:
        small.wait()
    raw = step_ref[...] + to_column(bias_ref[...])
    pad[pl.ds(0, heads), :] = jnp.maximum(raw, 0.0) + jnp.log(1.0 + jnp.exp(-jnp.abs(raw)))
    step_size = pad[...]
    rate = to_column(rate_ref[...])
    if padded > heads:
        rate = jnp.concatenate([rate, jnp.zeros((padded - heads, 1), F32)], axis=0)
    log_decay = -step_size * rate
    sums = dot(split(log_decay, 3), pairs[...], 1, 0)
    cumulative = sums[:padded] + sums[padded : 2 * padded] + sums[2 * padded :]
    middle = cumulative[:, half - 1 : half]
    last = cumulative[:, rows - 1 : rows]
    factor_in[...] = split(jnp.exp(middle - cumulative) * step_size, 2)

    starts = starts_ref[...].astype(F32).reshape(1, -1)
    offset = s * rows
    place = (offset + lax.broadcasted_iota(jnp.int32, (rows, 1), 0)).astype(F32)
    place_lane = (offset + lax.broadcasted_iota(jnp.int32, (1, rows), 1)).astype(F32)
    doc = jnp.sum(jnp.where(starts <= place, 1.0, 0.0), axis=1, keepdims=True)
    before = jnp.sum(jnp.where(starts <= (offset - 1).astype(F32), 1.0, 0.0), axis=1, keepdims=True)
    doc_end = doc[rows - 1 : rows, :]
    joined_end = jnp.where(doc_end == before, 1.0, 0.0)

    def per_channel(column):
        return jnp.sum(spread * column, axis=0, keepdims=True)

    link_own[...] = per_channel(jnp.exp(last)) * joined_end
    end_gate = per_channel(jnp.exp(last - middle))
    before_gate[1:2, :] = end_gate
    in_end = jnp.where(doc == doc_end, in_ref[...].astype(F32), 0.0).astype(BF16)

    loads[0].wait()
    loads[1].start()
    loads[2].start()

    def columns(k):
        return pl.ds(pl.multiple_of(k * width, width), width)

    def meet():
        greetings = len(peers) + 2 + (pair > 0).astype(jnp.int32) + (lent > 0).astype(jnp.int32)
        pl.semaphore_wait(barrier, greetings)

        @pl.when(carries & (pair > 0))
        def _():
            pl.semaphore_signal(ready_sem, inc=1, device_id=(s - 2, g), device_id_type=MESH)

        link_copy(1).start()

        @pl.when(core == 0)
        def _():
            link_copy(0).start()

        @pl.when(carries)
        def _():
            link_all[3] = link_own[...]

    def make_summary(k, _):
        cols = columns(k)
        scale = dot(factor_in[...], expand[:, cols], 0, 0)
        scaled = (stream[:, cols].astype(F32) * scale).astype(BF16)
        source[:, cols] = scaled
        fresh = dot(in_end, scaled, 0, 0) * before_gate[1:2, cols]

        for i in range(2):
            fresh_own[k, i] = fresh[:, i * sub : (i + 1) * sub].astype(BF16)
        @pl.when((k == 0) & carries)
        def _():
            meet()

        fresh_copy(k, 1).start()

        @pl.when(core == 0)
        def _():
            fresh_copy(k, 0).start()

        @pl.when(carries)
        def _():
            fresh_all[k, 3] = fresh_own[k, parity]

        return 0

    @pl.when(core == 0)
    def _():
        meet()

    lax.fori_loop(0, chunks, make_summary, 0)

    for small in smalls[5:]:
        small.wait()

    factor_out[...] = split(jnp.exp(cumulative - middle), 2)
    before_gate[3:4, :] = gain_ref[...].reshape(1, -1)
    doc_lane = jnp.sum(jnp.where(to_column(starts) <= place_lane, 1.0, 0.0), axis=0, keepdims=True)
    before_gate[0:1, :] = per_channel(jnp.exp(middle))
    skip = to_column(skip_ref[...])
    if padded > heads:
        skip = jnp.concatenate([skip, jnp.zeros((padded - heads, 1), F32)], axis=0)
    before_gate[2:3, :] = per_channel(skip)
    carry_in[...] = jnp.where(doc == before, out_ref[...].astype(F32), 0.0).astype(BF16)
    scores = dot(out_ref[...], in_ref[...], 1, 1)
    live = (first >= second) & (doc == doc_lane)
    pairs[...] = jnp.where(live, scores, 0.0).astype(BF16)
    square[...] = jnp.zeros_like(square)
    loads[1].wait()

    @pl.when(s == 0)
    def _():
        incoming_all[...] = jnp.zeros_like(incoming_all)

    def local_part(k):
        cols = columns(k)
        gate_value = gate[:, cols].astype(F32)
        silu = gate_value * (0.5 * jnp.tanh(0.5 * gate_value) + 0.5)
        within = jnp.concatenate(
            [
                dot(pairs[:half, :half], source[:half, cols], 1, 0),
                dot(pairs[half:, :], source[:, cols], 1, 0),
            ],
            axis=0,
        )
        factor = dot(factor_out[...], expand[:, cols], 0, 0) * silu
        slope[:, cols] = factor
        base[:, cols] = within * factor + stream[:, cols].astype(F32) * before_gate[2:3, cols] * silu

    def chain_step(k):
        cols = pl.ds(pl.multiple_of(k * width + parity * sub, sub), sub)

        @pl.when(k == 0)
        def _():
            arrived(link_all.at[pl.ds(0, 3)], link_recv)

        arrived(fresh_all.at[k, pl.ds(0, 3)], fresh_recv.at[k])

        for part in range(2):
            even, odd = 2 * part + 1 - parity, 2 * part + parity
            keep_even, keep_odd = link_all[even, :, cols], link_all[odd, :, cols]
            fresh_even = fresh_all[k, even].astype(F32)
            fresh_odd = fresh_all[k, odd].astype(F32)

            @pl.when(pair > 0)
            def _():
                chain_copy(k, part).wait_recv()
                between = keep_even * states[0, k, part].astype(F32) + fresh_even
                states[1, k, part] = between.astype(BF16)
                chain_out[k, part] = (keep_odd * between + fresh_odd).astype(BF16)

            @pl.when(pair == 0)
            def _():
                states[1, k, part] = fresh_all[k, even]
                chain_out[k, part] = (keep_odd * fresh_even + fresh_odd).astype(BF16)

            @pl.when(pair < last_pair)
            def _():
                chain_copy(k, part).start()

            @pl.when(cross > 0)
            def _():
                return_copy(k, 1, part, parity).start()

            @pl.when(s > 0)
            def _():
                if part == 0:
                    return_copy(k, 0, part, parity).start()
                else:
                    incoming_all[k, parity] = states[parity, k, part]

    def take(k):
        @pl.when(carries & (s > 0))
        def _():
            arrived(incoming_all.at[k, 0], return_recv.at[k])

        @pl.when((core == 0) & (s > 0))
        def _():
            arrived(incoming_all.at[k], return_recv.at[k])

    def half_rows(which):
        return pl.ds(pl.multiple_of(which * half, half), half)

    def piece_columns(j):
        return pl.ds(pl.multiple_of(j * piece, piece), piece)

    def finish(k, span):
        cols = columns(k)
        incoming = jnp.concatenate([incoming_all[k, i].astype(F32) for i in range(2)], axis=1)
        incoming = (incoming * before_gate[0:1, cols]).astype(BF16)
        carried = dot(carry_in[span, :], incoming, 1, 0)
        gated = base[span, cols] + slope[span, cols] * carried
        hidden[span, cols] = (gated * before_gate[3:4, cols]).astype(BF16)
        squares = gated * gated
        total = square[span, :]
        for i in range(width // 128):
            total = total + squares[:, i * 128 : (i + 1) * 128]
        square[span, :] = total

    def product(span, depth, j):
        return dot(hidden[span, depth], proj[depth, piece_columns(j)], 1, 0)

    early_depth = pl.ds(0, channels - width)
    late_depth = pl.ds(channels - width, width)

    lead = jnp.where(pair == 0, LEAD, chunks)


    def main_step(step, _):
        @pl.when(carries & (step >= lead) & (step < lead + chunks))
        def _():
            chain_step(step - lead)

        @pl.when(step < chunks)
        def _():
            local_part(step)

        @pl.when(carries & (step >= lead + LAG))
        def _():
            take(step - lead - LAG)
            finish(step - lead - LAG, pl.ds(0, rows))

        return 0

    @pl.when(carries & (pair < last_pair))
    def _():
        pl.semaphore_wait(ready_sem, 1)

    lax.fori_loop(0, chunks + jnp.where(carries, lead, 0), main_step, 0)

    loads[2].wait()

    def finish_step(k, _):
        take(k)
        finish(k, pl.ds(0, rows))
        return 0

    def near_copy(stage, j, sem):
        at = stage * pieces + j
        return remote(outbox.at[at], near_in.at[at], sent, sem, s, near)

    def place(j):
        return jnp.maximum(j - (pieces - 5), 0)

    def far_copy(j):
        return remote(outbox.at[2 * pieces + j], far_in.at[j], sent, far_recv.at[place(j)], s, far)

    def lend_copy(j):
        return remote(
            outbox.at[2 * pieces + j],
            relay_in.at[j - LEND_FROM],
            sent,
            relay_recv.at[j - LEND_FROM],
            helper,
            far,
        )

    def relay_copy(i):
        return remote(
            relay_in.at[i],
            far_in.at[i + LEND_FROM],
            relay_send,
            far_recv.at[place(i + LEND_FROM)],
            helper,
            g,
        )

    def core_rows(which):
        return pl.ds(pl.multiple_of(which * share, share), share)

    def extra_copy():
        return remote(outbox.at[3 * pieces], extra_in, sent, extra_recv, s, near)

    def extra_far_copy():
        return remote(
            outbox.at[3 * pieces], far_in.at[pieces - 1], sent, far_recv.at[4], s, 2 * (1 - side)
        )

    def exchange(stage, j):
        at = stage * pieces + j
        outbox[at] = held[at, core_rows(1 - core), :].astype(BF16)
        near_copy(stage, j, near_recv.at[j] if stage == 0 else near_last).start()

    def far_rows(which):
        return pl.ds(pl.multiple_of((1 - side) * half + which * share, share), share)

    def add_late(which):
        part = product(far_rows(which), late_depth, 0)
        held[0, core_rows(which), :] = held[0, core_rows(which), :] + part

    def project(stage, which, j):
        at = stage * pieces + j
        held[at] = product(half_rows(which), pl.ds(0, channels), j)

    def pass_on(j):
        near_copy(0, j, near_recv.at[j]).wait_recv()
        both = held[j, core_rows(core), :] + near_in[j].astype(F32)
        outbox[2 * pieces + j] = both.astype(BF16)
        lend = (j >= LEND_FROM) & (j < LEND_FROM + lent)

        @pl.when(lend)
        def _():
            lend_copy(j).start()

        @pl.when(jnp.logical_not(lend))
        def _():
            far_copy(j).start()

    def pass_on_extra():
        extra_copy().wait_recv()
        both = held[pieces - 1, core_rows(1 - core), :] + extra_in[...].astype(F32)
        outbox[3 * pieces] = both.astype(BF16)
        extra_far_copy().start()

    def square_copy(i):
        return remote(
            square_out.at[peers[i]], square_in.at[i], square_send, square_recv, s, peers[i]
        )

    def send_squares():
        for owner in range(n_head):
            block = square[owner * share : (owner + 1) * share, :]
            sums_lane = jnp.sum(block.T, axis=0, keepdims=True)
            square_out[owner] = sums_lane
        for i in range(len(peers)):
            square_copy(i).start()

    lax.fori_loop(jnp.where(carries, chunks - LAG, 0), chunks - 1, finish_step, 0)
    for j in range(READY):
        held[j] = product(half_rows(1 - side), early_depth, j)
    take(chunks - 1)
    finish(chunks - 1, far_rows(1 - core))
    add_late(1 - core)
    exchange(0, 0)
    finish(chunks - 1, far_rows(core))
    add_late(core)

    def far_step(j, _):
        @pl.when((j > 0) & (j < READY))
        def _():
            held[j] = held[j] + product(half_rows(1 - side), late_depth, j)

        @pl.when((j >= READY) & (j < pieces))
        def _():
            project(0, 1 - side, j)

        @pl.when(((j > 0) & (j < pieces - 1)) | ((j == pieces - 1) & (core == 0)))
        def _():
            exchange(0, j)

        @pl.when((j == pieces - 1) & (core == 0))
        def _():
            outbox[3 * pieces] = held[pieces - 1, core_rows(core), :].astype(BF16)
            extra_copy().start()

        @pl.when(j == SOON)
        def _():
            pass_on(0)
            finish(chunks - 1, half_rows(side))
            send_squares()

        @pl.when(carries & (j == pieces + FAR_LAG - 1))
        def _():
            pass_on_extra()

        @pl.when((j > FAR_LAG) & (carries | (j < pieces + FAR_LAG - 1)))
        def _():
            pass_on(j - FAR_LAG)

        return 0

    lax.fori_loop(0, pieces + FAR_LAG, far_step, 0)

    def near_step(j, _):
        project(1, side, j)
        exchange(1, j)
        return 0

    lax.fori_loop(0, pieces, near_step, 0)

    def relay_step(i, _):
        @pl.when(i < borrowed)
        def _():
            arrived(relay_in.at[i], relay_recv.at[i])
            relay_copy(i).start()

        return 0

    lax.fori_loop(0, SLOTS, relay_step, 0)

    arrived(square_in, square_recv)
    total = square_out[g]
    for i in range(len(peers)):
        total = total + square_in[i]
    mean = jnp.broadcast_to(total, (128, share)).T / (channels * n_head)
    scale_row = lax.rsqrt(mean + EPSILON)[:, 0:1]

    arrived(near_in.at[pl.ds(pieces, pieces)], near_last)

    arrived(far_in.at[pl.ds(0, pieces - 4)], far_recv.at[0])

    def collect(j, _):
        @pl.when(j > pieces - 5)
        def _():
            far_copy(j).wait_recv()

        at = pieces + j
        whole = held[at, core_rows(core), :] + near_in[at].astype(F32) + far_in[j].astype(F32)
        result_ref[:, piece_columns(j)] = (whole * scale_row).astype(BF16)
        return 0

    lax.fori_loop(0, pieces, collect, 0)

    link_copy(1).wait_send()

    @pl.when(core == 0)
    def _():
        link_copy(0).wait_send()
        left(fresh_own, fresh_send)

    @pl.when(carries)
    def _():
        left(fresh_own.at[:, 0], fresh_send)

    @pl.when(carries & (pair < last_pair))
    def _():
        left(chain_out, chain_send)

    @pl.when(carries & (cross > 0))
    def _():
        left(states.at[0], return_send.at[1])

    @pl.when(carries & (s > 0))
    def _():
        left(states.at[0, :, 0], return_send.at[0])

    left(square_out.at[pl.ds(0, 3)], square_send)
    left(outbox.at[pl.ds(0, 3 * pieces)], sent)

    for count in range(1, SLOTS + 1):

        @pl.when(borrowed == count)
        def _():
            left(relay_in.at[pl.ds(0, count)], relay_send)


def local(
    n_seq,
    n_head,
    stream,
    gate_input,
    in_coeff,
    out_coeff,
    step_raw,
    step_bias,
    decay_rate,
    skip_scale,
    norm_gain,
    out_proj,
    doc_starts,
):
    rows, channels = stream.shape
    heads = step_raw.shape[0]
    state = in_coeff.shape[1]
    model = out_proj.shape[1]
    chunks, pieces = channels // 256, model // 256
    width, piece = channels // chunks, model // pieces
    sub = width // 2
    padded = -(-heads // 8) * 8
    share = rows // n_head
    assert n_head == 4 and n_seq % 2 == 0 and rows <= 512
    vmem = pl.BlockSpec(memory_space=pltpu.VMEM)
    anywhere = pl.BlockSpec(memory_space=pl.ANY)
    dma = pltpu.SemaphoreType.DMA
    return pl.pallas_call(
        functools.partial(kernel, n_seq, n_head, heads, chunks, pieces),
        out_shape=pltpu.VMEM((share, model), BF16),
        in_specs=[anywhere] * 11,
        out_specs=vmem,
        scratch_shapes=[
            pltpu.VMEM(doc_starts.shape, doc_starts.dtype),
            pltpu.VMEM(step_raw.shape, F32),
            pltpu.VMEM((1, heads), F32),
            pltpu.VMEM((1, heads), F32),
            pltpu.VMEM((1, heads), F32),
            pltpu.VMEM(norm_gain.shape, F32),
            pltpu.VMEM(in_coeff.shape, BF16),
            pltpu.VMEM(out_coeff.shape, BF16),
            pltpu.VMEM((rows, channels), BF16),
            pltpu.VMEM((rows, channels), BF16),
            pltpu.VMEM((channels, model), BF16),
            pltpu.VMEM((padded, rows), F32),
            pltpu.VMEM((2 * padded, channels), BF16),
            pltpu.VMEM((2 * padded, rows), BF16),
            pltpu.VMEM((2 * padded, rows), BF16),
            pltpu.VMEM((rows, rows), BF16),
            pltpu.VMEM((rows, state), BF16),
            pltpu.VMEM((rows, channels), BF16),
            pltpu.VMEM((1, channels), F32),
            pltpu.VMEM((4, 1, channels), F32),
            pltpu.VMEM((8, channels), F32),
            pltpu.VMEM((rows, channels), F32),
            pltpu.VMEM((rows, channels), F32),
            pltpu.VMEM((rows, 128), F32),
            pltpu.VMEM((rows, channels), BF16),
            pltpu.VMEM((chunks, 2, state, sub), BF16),
            pltpu.VMEM((chunks, 4, state, sub), BF16),
            pltpu.VMEM((chunks, 2, state, sub), BF16),
            pltpu.VMEM((2, chunks, 2, state, sub), BF16),
            pltpu.VMEM((chunks, 2, state, sub), BF16),
            pltpu.VMEM((n_head, 1, share), F32),
            pltpu.VMEM((n_head - 1, 1, share), F32),
            pltpu.VMEM((2 * pieces, 2 * share, piece), F32),
            pltpu.VMEM((3 * pieces + 1, share, piece), BF16),
            pltpu.VMEM((2 * pieces, share, piece), BF16),
            pltpu.VMEM((pieces, share, piece), BF16),
            pltpu.VMEM((SLOTS, share, piece), BF16),
            pltpu.VMEM((share, piece), BF16),
            dma((8,)),
            dma((3,)),
            pltpu.SemaphoreType.REGULAR,
            dma((2,)),
            dma,
            dma,
            dma((chunks,)),
            dma,
            dma((chunks, 2)),
            dma((2,)),
            dma((chunks,)),
            dma,
            dma,
            dma,
            dma((pieces,)),
            dma,
            dma((5,)),
            dma,
            dma((SLOTS,)),
            dma,
        ],
        compiler_params=pltpu.CompilerParams(
            collective_id=0, has_side_effects=True, vmem_limit_bytes=56 * 1024 * 1024
        ),
    )(
        doc_starts,
        step_raw,
        step_bias.reshape(1, -1),
        decay_rate.reshape(1, -1),
        skip_scale.reshape(1, -1),
        norm_gain,
        in_coeff,
        out_coeff,
        stream,
        gate_input,
        out_proj,
    )


def solution(mesh):
    in_specs = (
        P("seq", "head"),
        P("seq", "head"),
        P("seq", None),
        P("seq", None),
        P("head", "seq"),
        P("head"),
        P("head"),
        P("head"),
        P("head"),
        P("head", None),
        P(),
    )
    out_specs = P(("seq", "head"), None)
    body = functools.partial(local, mesh.shape["seq"], mesh.shape["head"])
    return jax.shard_map(body, mesh=mesh, in_specs=in_specs, out_specs=out_specs, check_vma=False)
```

```python
import functools

import jax
import jax.numpy as jnp
from jax import lax
from jax.experimental import pallas as pl
from jax.experimental.pallas import tpu as pltpu
from jax.sharding import PartitionSpec as P

EPSILON = 1e-05
F32 = jnp.float32
BF16 = jnp.bfloat16
MESH = pl.DeviceIdType.MESH
LEAD = 1
LEND_FROM = 2
FAR_LAG = 2
READY = 2
SOON = 1
LAG = 4
LENT = ((2, 2), (0, 1))
SLOTS = max(max(counts) for counts in LENT)


def dot(a, b, ca, cb):
    return lax.dot_general(a, b, (((ca,), (cb,)), ((), ())), preferred_element_type=F32)


def split(value, parts):
    pieces = []
    for _ in range(parts):
        piece = value.astype(BF16).astype(F32)
        pieces.append(piece)
        value = value - piece
    return jnp.concatenate(pieces, axis=0).astype(BF16)


def to_column(row):
    n = row.shape[1]
    eye = lax.broadcasted_iota(jnp.int32, (n, n), 0) == lax.broadcasted_iota(jnp.int32, (n, n), 1)
    return jnp.sum(jnp.where(eye, row, 0.0), axis=1, keepdims=True)


def lends(pair, last_pair, core):
    if last_pair + 1 < 2 * len(LENT):
        return 0 * pair
    return sum(
        jnp.where(pair == last_pair - i, jnp.where(core == 0, *counts), 0)
        for i, counts in enumerate(LENT)
    )


def kernel(
    n_seq,
    n_head,
    heads,
    chunks,
    pieces,
    starts_hbm,
    step_hbm,
    bias_hbm,
    rate_hbm,
    skip_hbm,
    gain_hbm,
    in_hbm,
    out_hbm,
    stream_hbm,
    gate_hbm,
    proj_hbm,
    result_ref,
    starts_ref,
    step_ref,
    bias_ref,
    rate_ref,
    skip_ref,
    gain_ref,
    in_ref,
    out_ref,
    stream,
    gate,
    proj,
    pad,
    expand,
    factor_in,
    factor_out,
    pairs,
    carry_in,
    source,
    link_own,
    link_all,
    before_gate,
    base,
    slope,
    square,
    hidden,
    fresh_own,
    fresh_all,
    chain_out,
    states,
    incoming_all,
    square_out,
    square_in,
    held,
    outbox,
    near_in,
    far_in,
    relay_in,
    extra_in,
    small_sem,
    load_sem,
    ready_sem,
    link_send,
    link_recv,
    fresh_send,
    fresh_recv,
    chain_send,
    chain_recv,
    return_send,
    return_recv,
    square_send,
    square_recv,
    sent,
    near_recv,
    near_last,
    far_recv,
    relay_send,
    relay_recv,
    extra_recv,
):
    rows, channels = stream.shape
    state = in_ref.shape[1]
    width = channels // chunks
    head_size = channels // heads
    padded = pad.shape[0]
    sub = width // 2
    half = rows // 2
    share = rows // n_head
    piece = proj.shape[1] // pieces

    s = lax.axis_index("seq")
    g = lax.axis_index("head")
    parity = s % 2
    pair = s // 2
    last_pair = n_seq // 2 - 1
    core = g % 2
    side = g // 2
    near = side * 2 + (1 - core)
    far = (1 - side) * 2 + core
    cross = s + 1 - 2 * parity
    carrier = 2 * side + 1
    carries = core == 1
    helped = last_pair - pair
    lent = lends(pair, last_pair, core)
    borrowed = lends(helped, last_pair, core)
    helper = 2 * helped + parity
    peers = (near, far, (1 - side) * 2 + (1 - core))

    loads = [
        pltpu.make_async_copy(src, dst, load_sem.at[i])
        for i, (src, dst) in enumerate(((stream_hbm, stream), (gate_hbm, gate), (proj_hbm, proj)))
    ]
    smalls = [
        pltpu.make_async_copy(src, dst, small_sem.at[i])
        for i, (src, dst) in enumerate(
            (
                (step_hbm, step_ref),
                (bias_hbm, bias_ref),
                (rate_hbm, rate_ref),
                (starts_hbm, starts_ref),
                (in_hbm, in_ref),
                (skip_hbm, skip_ref),
                (gain_hbm, gain_ref),
                (out_hbm, out_ref),
            )
        )
    ]
    for small in smalls[:5]:
        small.start()
    loads[0].start()
    for small in smalls[5:]:
        small.start()

    barrier = pltpu.get_barrier_semaphore()
    for peer in peers:
        pl.semaphore_signal(barrier, inc=1, device_id=(s, peer), device_id_type=MESH)
    for peer in (g, near):
        pl.semaphore_signal(barrier, inc=1, device_id=(cross, peer), device_id_type=MESH)

    @pl.when(pair < last_pair)
    def _():
        pl.semaphore_signal(barrier, inc=1, device_id=(s + 2, g), device_id_type=MESH)

    @pl.when(borrowed > 0)
    def _():
        pl.semaphore_signal(barrier, inc=1, device_id=(helper, far), device_id_type=MESH)

    def remote(src, dst, send_sem, recv_sem, seq, head):
        return pltpu.make_async_remote_copy(
            src_ref=src,
            dst_ref=dst,
            send_sem=send_sem,
            recv_sem=recv_sem,
            device_id=(seq, head),
            device_id_type=MESH,
        )

    def slot(part, away):
        return 2 * part + 1 - away

    def link_copy(away):
        return remote(
            link_own,
            link_all.at[slot(core, away)],
            link_send.at[away],
            link_recv,
            cross if away else s,
            carrier,
        )

    def fresh_copy(k, away):
        return remote(
            fresh_own.at[k, 1 - parity if away else parity],
            fresh_all.at[k, slot(core, away)],
            fresh_send,
            fresh_recv.at[k],
            cross if away else s,
            carrier,
        )

    def chain_copy(k, part):
        return remote(
            chain_out.at[k, part],
            states.at[0, k, part],
            chain_send,
            chain_recv.at[k, part],
            (s + 2) % n_seq,
            g,
        )

    def return_copy(k, away, part, owner):
        return remote(
            states.at[1 - parity if away else parity, k, part],
            incoming_all.at[k, owner],
            return_send.at[away],
            return_recv.at[k],
            cross if away else s,
            2 * side + part,
        )

    def arrived(dst, sem):
        remote(dst, dst, sem, sem, s, near).wait_recv()

    def left(src, sem):
        remote(src, src, sem, sem, s, near).wait_send()

    pad[...] = jnp.zeros_like(pad)
    head_row = lax.broadcasted_iota(jnp.int32, (padded, channels), 0) * head_size
    lane = lax.broadcasted_iota(jnp.int32, (padded, channels), 1)
    spread = jnp.where((lane >= head_row) & (lane < head_row + head_size), 1.0, 0.0)
    expand[...] = jnp.concatenate([spread, spread], axis=0).astype(BF16)
    first = lax.broadcasted_iota(jnp.int32, (rows, rows), 0)
    second = lax.broadcasted_iota(jnp.int32, (rows, rows), 1)
    upper = jnp.where(first <= second, 1.0, 0.0).astype(BF16)
    pairs[...] = upper
    for small in smalls[:5]:
        small.wait()
    raw = step_ref[...] + to_column(bias_ref[...])
    pad[pl.ds(0, heads), :] = jnp.maximum(raw, 0.0) + jnp.log(1.0 + jnp.exp(-jnp.abs(raw)))
    step_size = pad[...]
    rate = to_column(rate_ref[...])
    if padded > heads:
        rate = jnp.concatenate([rate, jnp.zeros((padded - heads, 1), F32)], axis=0)
    log_decay = -step_size * rate
    sums = dot(split(log_decay, 3), pairs[...], 1, 0)
    cumulative = sums[:padded] + sums[padded : 2 * padded] + sums[2 * padded :]
    middle = cumulative[:, half - 1 : half]
    last = cumulative[:, rows - 1 : rows]
    factor_in[...] = split(jnp.exp(middle - cumulative) * step_size, 2)

    starts = starts_ref[...].astype(F32).reshape(1, -1)
    offset = s * rows
    place = (offset + lax.broadcasted_iota(jnp.int32, (rows, 1), 0)).astype(F32)
    place_lane = (offset + lax.broadcasted_iota(jnp.int32, (1, rows), 1)).astype(F32)
    doc = jnp.sum(jnp.where(starts <= place, 1.0, 0.0), axis=1, keepdims=True)
    before = jnp.sum(jnp.where(starts <= (offset - 1).astype(F32), 1.0, 0.0), axis=1, keepdims=True)
    doc_end = doc[rows - 1 : rows, :]
    joined_end = jnp.where(doc_end == before, 1.0, 0.0)

    def per_channel(column):
        return jnp.sum(spread * column, axis=0, keepdims=True)

    link_own[...] = per_channel(jnp.exp(last)) * joined_end
    end_gate = per_channel(jnp.exp(last - middle))
    before_gate[1:2, :] = end_gate
    in_end = jnp.where(doc == doc_end, in_ref[...].astype(F32), 0.0).astype(BF16)

    loads[0].wait()
    loads[1].start()
    loads[2].start()

    def columns(k):
        return pl.ds(pl.multiple_of(k * width, width), width)

    def meet():
        greetings = len(peers) + 2 + (pair > 0).astype(jnp.int32) + (lent > 0).astype(jnp.int32)
        pl.semaphore_wait(barrier, greetings)

        @pl.when(carries & (pair > 0))
        def _():
            pl.semaphore_signal(ready_sem, inc=1, device_id=(s - 2, g), device_id_type=MESH)

        link_copy(1).start()

        @pl.when(core == 0)
        def _():
            link_copy(0).start()

        @pl.when(carries)
        def _():
            link_all[3] = link_own[...]

    def make_summary(k, _):
        cols = columns(k)
        scale = dot(factor_in[...], expand[:, cols], 0, 0)
        scaled = (stream[:, cols].astype(F32) * scale).astype(BF16)
        source[:, cols] = scaled
        fresh = dot(in_end, scaled, 0, 0) * before_gate[1:2, cols]

        for i in range(2):
            fresh_own[k, i] = fresh[:, i * sub : (i + 1) * sub].astype(BF16)
        @pl.when((k == 0) & carries)
        def _():
            meet()

        fresh_copy(k, 1).start()

        @pl.when(core == 0)
        def _():
            fresh_copy(k, 0).start()

        @pl.when(carries)
        def _():
            fresh_all[k, 3] = fresh_own[k, parity]

        return 0

    @pl.when(core == 0)
    def _():
        meet()

    lax.fori_loop(0, chunks, make_summary, 0)

    for small in smalls[5:]:
        small.wait()

    factor_out[...] = split(jnp.exp(cumulative - middle), 2)
    before_gate[3:4, :] = gain_ref[...].reshape(1, -1)
    doc_lane = jnp.sum(jnp.where(to_column(starts) <= place_lane, 1.0, 0.0), axis=0, keepdims=True)
    before_gate[0:1, :] = per_channel(jnp.exp(middle))
    skip = to_column(skip_ref[...])
    if padded > heads:
        skip = jnp.concatenate([skip, jnp.zeros((padded - heads, 1), F32)], axis=0)
    before_gate[2:3, :] = per_channel(skip)
    carry_in[...] = jnp.where(doc == before, out_ref[...].astype(F32), 0.0).astype(BF16)
    scores = dot(out_ref[...], in_ref[...], 1, 1)
    live = (first >= second) & (doc == doc_lane)
    pairs[...] = jnp.where(live, scores, 0.0).astype(BF16)
    square[...] = jnp.zeros_like(square)
    loads[1].wait()

    @pl.when(s == 0)
    def _():
        incoming_all[...] = jnp.zeros_like(incoming_all)

    def local_part(k):
        cols = columns(k)
        gate_value = gate[:, cols].astype(F32)
        silu = gate_value * (0.5 * jnp.tanh(0.5 * gate_value) + 0.5)
        within = jnp.concatenate(
            [
                dot(pairs[:half, :half], source[:half, cols], 1, 0),
                dot(pairs[half:, :], source[:, cols], 1, 0),
            ],
            axis=0,
        )
        factor = dot(factor_out[...], expand[:, cols], 0, 0) * silu
        slope[:, cols] = factor
        base[:, cols] = within * factor + stream[:, cols].astype(F32) * before_gate[2:3, cols] * silu

    def chain_step(k):
        cols = pl.ds(pl.multiple_of(k * width + parity * sub, sub), sub)

        @pl.when(k == 0)
        def _():
            arrived(link_all.at[pl.ds(0, 3)], link_recv)

        arrived(fresh_all.at[k, pl.ds(0, 3)], fresh_recv.at[k])

        for part in range(2):
            even, odd = 2 * part + 1 - parity, 2 * part + parity
            keep_even, keep_odd = link_all[even, :, cols], link_all[odd, :, cols]
            fresh_even = fresh_all[k, even].astype(F32)
            fresh_odd = fresh_all[k, odd].astype(F32)

            @pl.when(pair > 0)
            def _():
                chain_copy(k, part).wait_recv()
                between = keep_even * states[0, k, part].astype(F32) + fresh_even
                states[1, k, part] = between.astype(BF16)
                chain_out[k, part] = (keep_odd * between + fresh_odd).astype(BF16)

            @pl.when(pair == 0)
            def _():
                states[1, k, part] = fresh_all[k, even]
                chain_out[k, part] = (keep_odd * fresh_even + fresh_odd).astype(BF16)

            @pl.when(pair < last_pair)
            def _():
                chain_copy(k, part).start()

            @pl.when(cross > 0)
            def _():
                return_copy(k, 1, part, parity).start()

            @pl.when(s > 0)
            def _():
                if part == 0:
                    return_copy(k, 0, part, parity).start()
                else:
                    incoming_all[k, parity] = states[parity, k, part]

    def take(k):
        @pl.when(carries & (s > 0))
        def _():
            arrived(incoming_all.at[k, 0], return_recv.at[k])

        @pl.when((core == 0) & (s > 0))
        def _():
            arrived(incoming_all.at[k], return_recv.at[k])

    def half_rows(which):
        return pl.ds(pl.multiple_of(which * half, half), half)

    def piece_columns(j):
        return pl.ds(pl.multiple_of(j * piece, piece), piece)

    def finish(k, span):
        cols = columns(k)
        incoming = jnp.concatenate([incoming_all[k, i].astype(F32) for i in range(2)], axis=1)
        incoming = (incoming * before_gate[0:1, cols]).astype(BF16)
        carried = dot(carry_in[span, :], incoming, 1, 0)
        gated = base[span, cols] + slope[span, cols] * carried
        hidden[span, cols] = (gated * before_gate[3:4, cols]).astype(BF16)
        squares = gated * gated
        total = square[span, :]
        for i in range(width // 128):
            total = total + squares[:, i * 128 : (i + 1) * 128]
        square[span, :] = total

    def product(span, depth, j):
        return dot(hidden[span, depth], proj[depth, piece_columns(j)], 1, 0)

    early_depth = pl.ds(0, channels - width)
    late_depth = pl.ds(channels - width, width)

    lead = jnp.where(pair == 0, LEAD, chunks)


    def main_step(step, _):
        @pl.when(carries & (step >= lead) & (step < lead + chunks))
        def _():
            chain_step(step - lead)

        @pl.when(step < chunks)
        def _():
            local_part(step)

        @pl.when(carries & (step >= lead + LAG))
        def _():
            take(step - lead - LAG)
            finish(step - lead - LAG, pl.ds(0, rows))

        return 0

    @pl.when(carries & (pair < last_pair))
    def _():
        pl.semaphore_wait(ready_sem, 1)

    lax.fori_loop(0, chunks + jnp.where(carries, lead, 0), main_step, 0)

    loads[2].wait()

    def finish_step(k, _):
        take(k)
        finish(k, pl.ds(0, rows))
        return 0

    def near_copy(stage, j, sem):
        at = stage * pieces + j
        return remote(outbox.at[at], near_in.at[at], sent, sem, s, near)

    def place(j):
        return jnp.maximum(j - (pieces - 5), 0)

    def far_copy(j):
        return remote(outbox.at[2 * pieces + j], far_in.at[j], sent, far_recv.at[place(j)], s, far)

    def lend_copy(j):
        return remote(
            outbox.at[2 * pieces + j],
            relay_in.at[j - LEND_FROM],
            sent,
            relay_recv.at[j - LEND_FROM],
            helper,
            far,
        )

    def relay_copy(i):
        return remote(
            relay_in.at[i],
            far_in.at[i + LEND_FROM],
            relay_send,
            far_recv.at[place(i + LEND_FROM)],
            helper,
            g,
        )

    def core_rows(which):
        return pl.ds(pl.multiple_of(which * share, share), share)

    def extra_copy():
        return remote(outbox.at[3 * pieces], extra_in, sent, extra_recv, s, near)

    def extra_far_copy():
        return remote(
            outbox.at[3 * pieces], far_in.at[pieces - 1], sent, far_recv.at[4], s, 2 * (1 - side)
        )

    def exchange(stage, j):
        at = stage * pieces + j
        outbox[at] = held[at, core_rows(1 - core), :].astype(BF16)
        near_copy(stage, j, near_recv.at[j] if stage == 0 else near_last).start()

    def far_rows(which):
        return pl.ds(pl.multiple_of((1 - side) * half + which * share, share), share)

    def add_late(which):
        part = product(far_rows(which), late_depth, 0)
        held[0, core_rows(which), :] = held[0, core_rows(which), :] + part

    def project(stage, which, j):
        at = stage * pieces + j
        held[at] = product(half_rows(which), pl.ds(0, channels), j)

    def pass_on(j):
        near_copy(0, j, near_recv.at[j]).wait_recv()
        both = held[j, core_rows(core), :] + near_in[j].astype(F32)
        outbox[2 * pieces + j] = both.astype(BF16)
        lend = (j >= LEND_FROM) & (j < LEND_FROM + lent)

        @pl.when(lend)
        def _():
            lend_copy(j).start()

        @pl.when(jnp.logical_not(lend))
        def _():
            far_copy(j).start()

    def pass_on_extra():
        extra_copy().wait_recv()
        both = held[pieces - 1, core_rows(1 - core), :] + extra_in[...].astype(F32)
        outbox[3 * pieces] = both.astype(BF16)
        extra_far_copy().start()

    def square_copy(i):
        return remote(
            square_out.at[peers[i]], square_in.at[i], square_send, square_recv, s, peers[i]
        )

    def send_squares():
        for owner in range(n_head):
            block = square[owner * share : (owner + 1) * share, :]
            sums_lane = jnp.sum(block.T, axis=0, keepdims=True)
            square_out[owner] = sums_lane
        for i in range(len(peers)):
            square_copy(i).start()

    lax.fori_loop(jnp.where(carries, chunks - LAG, 0), chunks - 1, finish_step, 0)
    for j in range(READY):
        held[j] = product(half_rows(1 - side), early_depth, j)
    take(chunks - 1)
    finish(chunks - 1, far_rows(1 - core))
    add_late(1 - core)
    exchange(0, 0)
    finish(chunks - 1, far_rows(core))
    add_late(core)

    def far_step(j, _):
        @pl.when((j > 0) & (j < READY))
        def _():
            held[j] = held[j] + product(half_rows(1 - side), late_depth, j)

        @pl.when((j >= READY) & (j < pieces))
        def _():
            project(0, 1 - side, j)

        @pl.when(((j > 0) & (j < pieces - 1)) | ((j == pieces - 1) & (core == 0)))
        def _():
            exchange(0, j)

        @pl.when((j == pieces - 1) & (core == 0))
        def _():
            outbox[3 * pieces] = held[pieces - 1, core_rows(core), :].astype(BF16)
            extra_copy().start()

        @pl.when(j == SOON)
        def _():
            pass_on(0)
            finish(chunks - 1, half_rows(side))
            send_squares()

        @pl.when(carries & (j == pieces + FAR_LAG - 1))
        def _():
            pass_on_extra()

        @pl.when((j > FAR_LAG) & (carries | (j < pieces + FAR_LAG - 1)))
        def _():
            pass_on(j - FAR_LAG)

        return 0

    lax.fori_loop(0, pieces + FAR_LAG, far_step, 0)

    def near_step(j, _):
        project(1, side, j)
        exchange(1, j)
        return 0

    lax.fori_loop(0, pieces, near_step, 0)

    def relay_step(i, _):
        @pl.when(i < borrowed)
        def _():
            arrived(relay_in.at[i], relay_recv.at[i])
            relay_copy(i).start()

        return 0

    lax.fori_loop(0, SLOTS, relay_step, 0)

    arrived(square_in, square_recv)
    total = square_out[g]
    for i in range(len(peers)):
        total = total + square_in[i]
    mean = jnp.broadcast_to(total, (128, share)).T / (channels * n_head)
    scale_row = lax.rsqrt(mean + EPSILON)[:, 0:1]

    arrived(near_in.at[pl.ds(pieces, pieces)], near_last)

    arrived(far_in.at[pl.ds(0, pieces - 4)], far_recv.at[0])

    def collect(j, _):
        @pl.when(j > pieces - 5)
        def _():
            far_copy(j).wait_recv()

        at = pieces + j
        whole = held[at, core_rows(core), :] + near_in[at].astype(F32) + far_in[j].astype(F32)
        result_ref[:, piece_columns(j)] = (whole * scale_row).astype(BF16)
        return 0

    lax.fori_loop(0, pieces, collect, 0)

    link_copy(1).wait_send()

    @pl.when(core == 0)
    def _():
        link_copy(0).wait_send()
        left(fresh_own, fresh_send)

    @pl.when(carries)
    def _():
        left(fresh_own.at[:, 0], fresh_send)

    @pl.when(carries & (pair < last_pair))
    def _():
        left(chain_out, chain_send)

    @pl.when(carries & (cross > 0))
    def _():
        left(states.at[0], return_send.at[1])

    @pl.when(carries & (s > 0))
    def _():
        left(states.at[0, :, 0], return_send.at[0])

    left(square_out.at[pl.ds(0, 3)], square_send)
    left(outbox.at[pl.ds(0, 3 * pieces)], sent)

    for count in range(1, SLOTS + 1):

        @pl.when(borrowed == count)
        def _():
            left(relay_in.at[pl.ds(0, count)], relay_send)


def local(
    n_seq,
    n_head,
    stream,
    gate_input,
    in_coeff,
    out_coeff,
    step_raw,
    step_bias,
    decay_rate,
    skip_scale,
    norm_gain,
    out_proj,
    doc_starts,
):
    rows, channels = stream.shape
    heads = step_raw.shape[0]
    state = in_coeff.shape[1]
    model = out_proj.shape[1]
    chunks, pieces = channels // 256, model // 256
    width, piece = channels // chunks, model // pieces
    sub = width // 2
    padded = -(-heads // 8) * 8
    share = rows // n_head
    assert n_head == 4 and n_seq % 2 == 0 and rows <= 512
    vmem = pl.BlockSpec(memory_space=pltpu.VMEM)
    anywhere = pl.BlockSpec(memory_space=pl.ANY)
    dma = pltpu.SemaphoreType.DMA
    return pl.pallas_call(
        functools.partial(kernel, n_seq, n_head, heads, chunks, pieces),
        out_shape=pltpu.VMEM((share, model), BF16),
        in_specs=[anywhere] * 11,
        out_specs=vmem,
        scratch_shapes=[
            pltpu.VMEM(doc_starts.shape, doc_starts.dtype),
            pltpu.VMEM(step_raw.shape, F32),
            pltpu.VMEM((1, heads), F32),
            pltpu.VMEM((1, heads), F32),
            pltpu.VMEM((1, heads), F32),
            pltpu.VMEM(norm_gain.shape, F32),
            pltpu.VMEM(in_coeff.shape, BF16),
            pltpu.VMEM(out_coeff.shape, BF16),
            pltpu.VMEM((rows, channels), BF16),
            pltpu.VMEM((rows, channels), BF16),
            pltpu.VMEM((channels, model), BF16),
            pltpu.VMEM((padded, rows), F32),
            pltpu.VMEM((2 * padded, channels), BF16),
            pltpu.VMEM((2 * padded, rows), BF16),
            pltpu.VMEM((2 * padded, rows), BF16),
            pltpu.VMEM((rows, rows), BF16),
            pltpu.VMEM((rows, state), BF16),
            pltpu.VMEM((rows, channels), BF16),
            pltpu.VMEM((1, channels), F32),
            pltpu.VMEM((4, 1, channels), F32),
            pltpu.VMEM((8, channels), F32),
            pltpu.VMEM((rows, channels), F32),
            pltpu.VMEM((rows, channels), F32),
            pltpu.VMEM((rows, 128), F32),
            pltpu.VMEM((rows, channels), BF16),
            pltpu.VMEM((chunks, 2, state, sub), BF16),
            pltpu.VMEM((chunks, 4, state, sub), BF16),
            pltpu.VMEM((chunks, 2, state, sub), BF16),
            pltpu.VMEM((2, chunks, 2, state, sub), BF16),
            pltpu.VMEM((chunks, 2, state, sub), BF16),
            pltpu.VMEM((n_head, 1, share), F32),
            pltpu.VMEM((n_head - 1, 1, share), F32),
            pltpu.VMEM((2 * pieces, 2 * share, piece), F32),
            pltpu.VMEM((3 * pieces + 1, share, piece), BF16),
            pltpu.VMEM((2 * pieces, share, piece), BF16),
            pltpu.VMEM((pieces, share, piece), BF16),
            pltpu.VMEM((SLOTS, share, piece), BF16),
            pltpu.VMEM((share, piece), BF16),
            dma((8,)),
            dma((3,)),
            pltpu.SemaphoreType.REGULAR,
            dma((2,)),
            dma,
            dma,
            dma((chunks,)),
            dma,
            dma((chunks, 2)),
            dma((2,)),
            dma((chunks,)),
            dma,
            dma,
            dma,
            dma((pieces,)),
            dma,
            dma((5,)),
            dma,
            dma((SLOTS,)),
            dma,
        ],
        compiler_params=pltpu.CompilerParams(
            collective_id=0, has_side_effects=True, vmem_limit_bytes=56 * 1024 * 1024
        ),
    )(
        doc_starts,
        step_raw,
        step_bias.reshape(1, -1),
        decay_rate.reshape(1, -1),
        skip_scale.reshape(1, -1),
        norm_gain,
        in_coeff,
        out_coeff,
        stream,
        gate_input,
        out_proj,
    )


def solution(mesh):
    in_specs = (
        P("seq", "head"),
        P("seq", "head"),
        P("seq", None),
        P("seq", None),
        P("head", "seq"),
        P("head"),
        P("head"),
        P("head"),
        P("head"),
        P("head", None),
        P(),
    )
    out_specs = P(("seq", "head"), None)
    body = functools.partial(local, mesh.shape["seq"], mesh.shape["head"])
    return jax.shard_map(body, mesh=mesh, in_specs=in_specs, out_specs=out_specs, check_vma=False)
```
